256 devices in a mesh: seq: 128 (over z, x_hi, y, core), mp: 2 (over x_lo).
Axes of the slice: x: 4 (x_hi: 2, x_lo: 2; x = x_hi * 2 + x_lo), y: 4, z: 8, core: 2. Of those that a mesh axis runs over, the one named last changes fastest.
Arguments:
- stream: bfloat16 [16384, 8192], P('seq', 'mp'), may hold values from -17 to 17
- norm_gain: float32 [8192], P('mp'), may hold values from 0.5 to 1.5
- short_outer: bfloat16 [16384, 8192], P('seq', 'mp'), may hold values from -4 to 4
- short_inner: bfloat16 [16384, 8192], P('seq', 'mp'), may hold values from -4 to 4
- short_filter: bfloat16 [128, 8192], P(None, 'mp'), may hold values from -0.5 to 0.5
- long_outer: bfloat16 [16384, 8192], P('seq', 'mp'), may hold values from -4 to 4
- long_inner: bfloat16 [16384, 8192], P('seq', 'mp'), may hold values from -4 to 4
- long_decay: float32 [8192], P('mp'), may hold values from 1e-06 to 0.03
- query_heads: bfloat16 [16384, 8192], P('seq', 'mp'), may hold values from -6 to 6
- key_heads: bfloat16 [16384, 8192], P('seq', 'mp'), may hold values from -6 to 6
Outputs:
- long_mixed: bfloat16 [16384, 8192], P('seq', 'mp')
- attended: bfloat16 [16384, 8192], P('seq', 'mp')
The draws below stay inside these ranges and needn't reach their ends.
All inputs are finite; a program needn't handle non-finite values.
Results may differ from the reference program's by a relative error of at most 0.013.
Values may be sent and summed in bfloat16 or wider, within the bound.
No kernel may reach another device: no remote copies, remote signals or barrier semaphores. Data moves between devices by JAX's collectives and lax.ppermute only.
A program may use at most 64 MiB of HBM per device.

```python
import math
import jax
import jax.numpy as jnp
from jax import lax

D = 8192
HEADS = 64
HEAD_DIM = 128
TAPS = 128
TOK_DEV = 128
SEQ_LEN = 16384
N_SEQ = 128


def draw_stream(key, part):
    shape = (SEQ_LEN, D // 128, 128)
    base = jnp.clip(jax.random.normal(jax.random.fold_in(key, 11), shape, jnp.float32), -4.0, 4.0)
    levels = jnp.exp(jax.random.uniform(jax.random.fold_in(key, 13), (SEQ_LEN, D // 128, 1), jnp.float32, -1.4, 1.4))
    return (base * levels).reshape(SEQ_LEN, D).astype(jnp.bfloat16)


def draw_long_decay(key, part):
    upper = math.log(0.03)
    return jnp.exp(jax.random.uniform(jax.random.fold_in(key, 41), (D,), jnp.float32, math.log(1e-06), upper))


def draw_heads(key, salt):
    drawn = jnp.clip(jax.random.normal(jax.random.fold_in(key, salt), (SEQ_LEN, D), jnp.float32), -6.0, 6.0)
    return drawn


def draw_query_heads(key, part):
    return draw_heads(key, 31).astype(jnp.bfloat16)


def draw_key_heads(key, part):
    return draw_heads(key, 32).astype(jnp.bfloat16)


def block_scale(rng, extent, split, low, high):
    loudness, own = 1.0, jax.random.fold_in(rng, 6)
    for axis_at, parts in split:
        heights = jnp.exp(jax.random.uniform(jax.random.fold_in(own, axis_at), (parts,), jnp.float32, low / len(split), high / len(split)))
        loudness = loudness * jnp.repeat(heights, extent[axis_at] // parts).reshape([-1 if axis == axis_at else 1 for axis in range(len(extent))])
    return loudness


def normal_values(key, extent, width, most, cuts=(), kind=jnp.bfloat16):
    values = width * jax.random.normal(key, extent, jnp.float32)
    if cuts:
        values = values * block_scale(key, extent, cuts, -0.22, 0.18)
    return jnp.clip(values, -most, most).astype(kind)


def setup_inputs(seed: int = 0) -> dict:
    key_list = jax.random.split(jax.random.key(seed), 11)
    stream = draw_stream(jax.random.fold_in(key_list[10], 71), 0)
    norm_gain = jnp.clip(1.0 + 0.1 * jax.random.normal(key_list[1], (D,), jnp.float32), 0.5, 1.5)
    short_outer = normal_values(key_list[2], (SEQ_LEN, D), 1.0, 4.0, ((0, 128), (1, 2)))
    short_inner = normal_values(key_list[3], (SEQ_LEN, D), 1.0, 4.0, ((0, 128), (1, 2)))
    short_filter = normal_values(key_list[4], (TAPS, D), TAPS ** -0.5, 0.5, ((1, 2),))
    long_outer = normal_values(key_list[5], (SEQ_LEN, D), 1.0, 4.0, ((0, 128), (1, 2)))
    long_inner = normal_values(key_list[6], (SEQ_LEN, D), 1.0, 4.0, ((0, 128), (1, 2)))
    long_decay = draw_long_decay(jax.random.fold_in(key_list[10], 71), 0)
    query_heads = draw_query_heads(jax.random.fold_in(key_list[10], 71), 0)
    key_heads = draw_key_heads(jax.random.fold_in(key_list[10], 71), 0)
    return {"stream": stream, "norm_gain": norm_gain, "short_outer": short_outer, "short_inner": short_inner, "short_filter": short_filter, "long_outer": long_outer, "long_inner": long_inner, "long_decay": long_decay, "query_heads": query_heads, "key_heads": key_heads}


def pair_combine(first_pair, second_pair):
    return (first_pair[0] * second_pair[0], second_pair[0] * first_pair[1] + second_pair[1])

def reference(stream, norm_gain, short_outer, short_inner, short_filter, long_outer, long_inner, long_decay, query_heads, key_heads):
    rates = jnp.exp(-long_decay)
    scales = jnp.sqrt(-jnp.expm1(-2.0 * long_decay))
    filt = short_filter.astype(jnp.float32)

    def blocked(array):
        return array.reshape(N_SEQ, TOK_DEV, D)
    inputs = (jnp.arange(N_SEQ, dtype=jnp.int32), blocked(stream), blocked(short_outer), blocked(short_inner), blocked(long_outer), blocked(long_inner), blocked(query_heads), blocked(key_heads))

    def block_step(carry, pieces):
        tail, state, prev_keys, prev_values = carry
        block_index, x_blk, s_outer, s_inner, l_outer, l_inner, q_blk, k_blk = pieces
        x_float = x_blk.astype(jnp.float32)
        mean_square = lax.optimization_barrier(jnp.mean(x_float * x_float, axis=1, keepdims=True))
        normed = x_float * norm_gain / jnp.sqrt(mean_square + 0.5)
        short_in = (s_inner.astype(jnp.float32) * normed).astype(jnp.bfloat16)
        extended = jnp.concatenate([tail, short_in], axis=0).astype(jnp.float32)

        def tap_step(j, acc):
            start = (TAPS - 1 - j).astype(jnp.int32)
            window = lax.dynamic_slice_in_dim(extended, start, TOK_DEV, 0)
            return acc + lax.dynamic_slice_in_dim(filt, j.astype(jnp.int32), 1, 0) * window
        short_conv = lax.fori_loop(0, TAPS, tap_step, jnp.zeros((TOK_DEV, D), jnp.float32))
        long_in = (l_inner.astype(jnp.float32) * s_outer.astype(jnp.float32) * short_conv).astype(jnp.bfloat16)
        factors = jnp.broadcast_to(rates, long_in.shape)
        powers, states = lax.associative_scan(pair_combine, (factors, long_in.astype(jnp.float32)), axis=0)
        states = states + powers * state
        long_mixed = (l_outer.astype(jnp.float32) * (states * scales)).astype(jnp.bfloat16)
        query = q_blk.astype(jnp.float32).reshape(TOK_DEV, HEADS, HEAD_DIM)
        keys = jnp.concatenate([prev_keys, k_blk], axis=0).astype(jnp.float32).reshape(2 * TOK_DEV, HEADS, HEAD_DIM)
        values = jnp.concatenate([prev_values, long_mixed], axis=0).astype(jnp.float32).reshape(2 * TOK_DEV, HEADS, HEAD_DIM)
        scores = jnp.einsum('thd,shd->hts', query, keys) * HEAD_DIM ** (-0.5)
        row_pos = jnp.arange(TOK_DEV, dtype=jnp.int32)[:, None]
        col_pos = jnp.arange(2 * TOK_DEV, dtype=jnp.int32)[None, :]
        valid = (col_pos <= row_pos + TOK_DEV) & ((col_pos >= TOK_DEV) | (block_index > 0))
        scores = jnp.where(valid[None], scores, -1e+30)
        weights = jax.nn.softmax(scores, axis=-1).astype(jnp.bfloat16)
        result = jnp.einsum('hts,shd->thd', weights.astype(jnp.float32), values)
        attended = result.reshape(TOK_DEV, D).astype(jnp.bfloat16)
        new_carry = (short_in[TOK_DEV - (TAPS - 1):], states[-1], k_blk, long_mixed)
        return (new_carry, (long_mixed, attended))
    start_carry = (jnp.zeros((TAPS - 1, D), jnp.bfloat16), jnp.zeros((D,), jnp.float32), jnp.zeros((TOK_DEV, D), jnp.bfloat16), jnp.zeros((TOK_DEV, D), jnp.bfloat16))
    _, outputs = lax.scan(block_step, start_carry, inputs)
    long_mixed = outputs[0].reshape(SEQ_LEN, D)
    attended = outputs[1].reshape(SEQ_LEN, D)
    return (long_mixed, attended)
```

```python
import jax
import jax.numpy as jnp
import numpy as np
from jax import lax
from jax.experimental import pallas as pl
from jax.experimental.pallas import tpu as pltpu
from jax.sharding import Mesh
from jax.sharding import PartitionSpec as P

D = 8192
HEAD_DIM = 128
BLOCK = 128
SEQ = ("seq_0", "seq_1", "seq_2", "seq_3")
NEAR = ("seq_2", "seq_3")
FAR = ("seq_0", "seq_1")
F32 = jnp.float32
BF16 = jnp.bfloat16
SUB = 256


def dft_matrices():
    n = 2 * BLOCK
    k = np.arange(BLOCK, dtype=np.float64)[:, None]
    t = np.arange(n, dtype=np.float64)[None, :]
    angle = np.pi * (2 * k + 1) * t / n
    forward = np.concatenate([np.cos(angle), -np.sin(angle)], axis=0)
    back = np.concatenate([np.cos(angle), -np.sin(angle)], axis=0).T[BLOCK:] * (2.0 / n)
    return forward.astype(np.float32), back.astype(np.float32)


FORWARD, BACK = dft_matrices()


def split(value):
    high = value.astype(BF16)
    return high, (value - high.astype(F32)).astype(BF16)


def dot(a, b):
    return jnp.dot(a, b, preferred_element_type=F32)


def shifted(block, axis, distance):
    size = lax.axis_size(axis)
    return lax.ppermute(block, axis, [(i, i + distance) for i in range(size - distance)])


def copies(array, axis):
    sent = jnp.broadcast_to(array, (lax.axis_size(axis), *array.shape))
    return lax.all_to_all(sent, axis, split_axis=0, concat_axis=0, tiled=True)


def gate_body(stream, inner, gain, v, squares, acc):
    step = pl.program_id(0)
    x = stream[...].astype(F32)
    v[...] = (inner[...].astype(F32) * x * gain[...]).astype(BF16)
    sq = x * x
    part = sq[:, :128]
    for j in range(1, x.shape[1] // 128):
        part = part + sq[:, j * 128 : (j + 1) * 128]

    @pl.when(step == 0)
    def _():
        acc[...] = part

    @pl.when(step > 0)
    def _():
        acc[...] = acc[...] + part

    @pl.when(step == pl.num_programs(0) - 1)
    def _():
        squares[...] = jnp.sum(acc[...].T, axis=0, keepdims=True)


def gated(stream, inner, gain, tile=1024):
    rows, width = stream.shape
    wide = pl.BlockSpec((rows, tile), lambda i: (0, i))
    return pl.pallas_call(
        gate_body,
        grid=(width // tile,),
        in_specs=[wide, wide, pl.BlockSpec((1, tile), lambda i: (0, i))],
        out_specs=[wide, pl.BlockSpec((1, rows), lambda i: (0, 0))],
        out_shape=[
            jax.ShapeDtypeStruct((rows, width), BF16),
            jax.ShapeDtypeStruct((1, rows), F32),
        ],
        scratch_shapes=[pltpu.VMEM((rows, 128), F32)],
        name="gated",
    )(stream, inner, gain)


def conv_body(
    before, here, taps, factor, forward, back, lower, inner, outer, decay, local, state, fr_hi, fr_lo
):
    step = pl.program_id(0)

    @pl.when(step == 0)
    def _():
        hi, lo = split(forward[...] * factor[...])
        fr_hi[...] = hi
        fr_lo[...] = lo

    f_hi, f_lo = split(forward[:, :BLOCK])
    b_hi, b_lo = split(back[...])
    for j in range(here.shape[1] // SUB):
        at = slice(j * SUB, (j + 1) * SUB)
        s = jnp.concatenate([before[:, at], here[:, at]], axis=0)
        x = dot(fr_hi[...], s) + dot(fr_lo[...], s)
        f = taps[:, at]
        h = dot(f_hi, f) + dot(f_lo, f)
        x_re, x_im = x[:BLOCK], x[BLOCK:]
        h_re, h_im = h[:BLOCK], h[BLOCK:]
        y = jnp.concatenate([x_re * h_re - x_im * h_im, x_re * h_im + x_im * h_re], axis=0)
        y_hi, y_lo = split(y)
        conv = dot(b_hi, y_hi) + dot(b_hi, y_lo) + dot(b_lo, y_hi)
        long_in = (inner[:, at].astype(F32) * outer[:, at].astype(F32) * conv).astype(BF16)
        d = decay[:, at]
        time = lax.broadcasted_iota(jnp.int32, (BLOCK, SUB), 0).astype(F32)
        z_hi, z_lo = split(long_in.astype(F32) * jnp.exp(d * time))
        total = dot(lower[...], z_hi) + dot(lower[...], z_lo)
        result = total * jnp.exp(-d * time)
        local[:, at] = result
        state[:, at] = result[BLOCK - 1 :]


def conv_scan(before, here, taps, factor, inner, outer, decay, tile=1024):
    rows, width = here.shape
    wide = pl.BlockSpec((rows, tile), lambda i: (0, i))
    row = pl.BlockSpec((1, tile), lambda i: (0, i))
    whole = lambda shape: pl.BlockSpec(shape, lambda i: (0, 0))
    lower = jnp.asarray(np.tril(np.ones((rows, rows), np.float32)), BF16)
    return pl.pallas_call(
        conv_body,
        grid=(width // tile,),
        in_specs=[
            wide,
            wide,
            wide,
            whole((1, 2 * rows)),
            whole((2 * rows, 2 * rows)),
            whole((rows, 2 * rows)),
            whole((rows, rows)),
            wide,
            wide,
            row,
        ],
        out_specs=[wide, row],
        out_shape=[
            jax.ShapeDtypeStruct((rows, width), F32),
            jax.ShapeDtypeStruct((1, width), F32),
        ],
        scratch_shapes=[pltpu.VMEM((2 * rows, 2 * rows), BF16)] * 2,
        name="conv_scan",
    )(before, here, taps, factor, jnp.asarray(FORWARD), jnp.asarray(BACK), lower, inner, outer, decay)


def mix_body(local, outer, decay, scale, carry, mixed):
    d = decay[...]
    time = lax.broadcasted_iota(jnp.int32, local.shape, 0).astype(F32)
    state = local[...] + jnp.exp(-d * (time + 1.0)) * carry[...]
    mixed[...] = (outer[...].astype(F32) * (state * scale[...])).astype(BF16)


def mix(local, outer, decay, scale, carry, tile=1024):
    rows, width = local.shape
    wide = pl.BlockSpec((rows, tile), lambda i: (0, i))
    row = pl.BlockSpec((1, tile), lambda i: (0, i))
    return pl.pallas_call(
        mix_body,
        grid=(width // tile,),
        in_specs=[wide, wide, row, row, row],
        out_specs=wide,
        out_shape=jax.ShapeDtypeStruct((rows, width), BF16),
        name="mix",
    )(local, outer, decay, scale, carry)


def weigh_body(first, query, key_before, key_here, weights):
    rows = query.shape[0]
    row_pos = lax.broadcasted_iota(jnp.int32, (rows, 2 * rows), 0)
    col_pos = lax.broadcasted_iota(jnp.int32, (rows, 2 * rows), 1)
    lowest = jnp.where(first[0] > 0, rows, 0)
    valid = (col_pos <= row_pos + rows) & (col_pos >= lowest)
    for j in range(query.shape[1] // HEAD_DIM):
        at = slice(j * HEAD_DIM, (j + 1) * HEAD_DIM)
        keys = jnp.concatenate([key_before[:, at], key_here[:, at]], axis=0)
        scores = lax.dot_general(
            query[:, at], keys, (((1,), (1,)), ((), ())), preferred_element_type=F32
        ) * HEAD_DIM ** (-0.5)
        scores = jnp.where(valid, scores, -1e30)
        top = jnp.max(scores, axis=1, keepdims=True)
        e = jnp.exp(scores - top)
        weights[j] = (e * (1.0 / jnp.sum(e, axis=1, keepdims=True))).astype(BF16)


def weigh(first, query, key_before, key_here, tile=1024):
    rows, width = query.shape
    heads = tile // HEAD_DIM
    wide = pl.BlockSpec((rows, tile), lambda i: (0, i))
    return pl.pallas_call(
        weigh_body,
        grid=(width // tile,),
        in_specs=[pl.BlockSpec(memory_space=pltpu.SMEM), wide, wide, wide],
        out_specs=pl.BlockSpec((heads, rows, 2 * rows), lambda i: (i, 0, 0)),
        out_shape=jax.ShapeDtypeStruct((width // HEAD_DIM, rows, 2 * rows), BF16),
        cost_estimate=pl.CostEstimate(flops=4 * 10**9, transcendentals=10**6, bytes_accessed=5 * 10**6),
        name="weigh",
    )(first, query, key_before, key_here)


def attend_body(weights, before, here, out):
    for j in range(weights.shape[0]):
        at = slice(j * HEAD_DIM, (j + 1) * HEAD_DIM)
        values = jnp.concatenate([before[:, at], here[:, at]], axis=0)
        out[:, at] = dot(weights[j], values).astype(BF16)


def attend(weights, before, here, tile=1024):
    rows, width = here.shape
    heads = tile // HEAD_DIM
    wide = pl.BlockSpec((rows, tile), lambda i: (0, i))
    return pl.pallas_call(
        attend_body,
        grid=(width // tile,),
        in_specs=[pl.BlockSpec((heads, rows, 2 * rows), lambda i: (i, 0, 0)), wide, wide],
        out_specs=wide,
        out_shape=jax.ShapeDtypeStruct((rows, width), BF16),
        name="attend",
    )(weights, before, here)


def weighted(pieces, place, rate):
    size = pieces.shape[0]
    pieces = pieces.astype(F32)
    k = lax.broadcasted_iota(jnp.int32, (size, 1, 1), 0)
    gap = place - 1 - k
    inside = jnp.where(gap >= 0, jnp.exp(-rate * jnp.maximum(gap, 0).astype(F32)), 0.0)
    return jnp.sum(inside * pieces, axis=0)


def on_device(
    stream,
    norm_gain,
    short_outer,
    short_inner,
    short_filter,
    long_outer,
    long_inner,
    long_decay,
    query_heads,
    key_heads,
):
    rows, width = stream.shape
    decay = long_decay[None]
    scale = jnp.sqrt(-jnp.expm1(-2.0 * decay))
    v, squares = gated(stream, short_inner, norm_gain[None])
    squares_before = shifted(squares, SEQ, 1)
    v, squares_before = lax.optimization_barrier((v, squares_before))
    v_before = shifted(v, SEQ, 1)
    both = jnp.concatenate([squares_before, squares], axis=1)
    totals = jnp.sum(copies(both, "mp"), axis=0)
    factor = 1.0 / jnp.sqrt(totals / D + 0.5)
    keys, factor = lax.optimization_barrier((key_heads, factor))
    key_before = shifted(keys, SEQ, 1)
    local, state = conv_scan(
        v_before, v, short_filter, factor, long_inner, short_outer, decay
    )
    near, far = lax.axis_index(NEAR), lax.axis_index(FAR)
    near_size = lax.axis_size(NEAR)
    rate = long_decay.reshape(width // 128, 128) * rows
    pieces = copies(state.reshape(width // 128, 128).astype(BF16), NEAR)
    group = weighted(pieces, near_size, rate)
    others = copies(group.astype(BF16), FAR)
    entering = weighted(pieces, near, rate) + jnp.exp(-rate * near.astype(F32)) * weighted(
        others, far, rate * near_size
    )
    mixed = mix(local, long_outer, decay, scale, entering.reshape(1, width))
    mixed_before = shifted(mixed, SEQ, 1)
    first = (lax.axis_index(SEQ) == 0).astype(jnp.int32)[None]
    weights = weigh(first, query_heads, key_before, key_heads)
    attended = attend(weights, mixed_before, mixed)
    return (mixed, attended)


def solution(mesh):
    finer = Mesh(
        mesh.devices.reshape(8, 2, 4, 2, mesh.shape["mp"]),
        ("seq_0", "seq_1", "seq_2", "seq_3", "mp"),
    )
    placed = (
        P(SEQ, "mp"),
        P("mp"),
        P(SEQ, "mp"),
        P(SEQ, "mp"),
        P(None, "mp"),
        P(SEQ, "mp"),
        P(SEQ, "mp"),
        P("mp"),
        P(SEQ, "mp"),
        P(SEQ, "mp"),
    )
    return jax.shard_map(
        on_device,
        mesh=finer,
        in_specs=placed,
        out_specs=(P(SEQ, "mp"), P(SEQ, "mp")),
        check_vma=False,
    )
```

```python
import jax
import jax.numpy as jnp
import numpy as np
from jax import lax
from jax.experimental import pallas as pl
from jax.experimental.pallas import tpu as pltpu
from jax.sharding import Mesh
from jax.sharding import PartitionSpec as P

D = 8192
HEAD_DIM = 128
BLOCK = 128
SEQ = ("seq_0", "seq_1", "seq_2", "seq_3")
NEAR = ("seq_2", "seq_3")
FAR = ("seq_0", "seq_1")
F32 = jnp.float32
BF16 = jnp.bfloat16
SUB = 256
VMEM = 8 * 2**20


def dft_matrices():
    n = 2 * BLOCK
    k = np.arange(BLOCK, dtype=np.float64)[:, None]
    t = np.arange(n, dtype=np.float64)[None, :]
    angle = np.pi * (2 * k + 1) * t / n
    forward = np.concatenate([np.cos(angle), -np.sin(angle)], axis=0)
    back = np.concatenate([np.cos(angle), -np.sin(angle)], axis=0).T[BLOCK:] * (2.0 / n)
    return forward.astype(np.float32), back.astype(np.float32)


FORWARD, BACK = dft_matrices()


def split(value):
    high = value.astype(BF16)
    return high, (value - high.astype(F32)).astype(BF16)


def dot(a, b):
    return jnp.dot(a, b, preferred_element_type=F32)


def shifted(block, axis, distance):
    size = lax.axis_size(axis)
    return lax.ppermute(block, axis, [(i, i + distance) for i in range(size) if 0 <= i + distance < size])


def copies(array, axis):
    sent = jnp.broadcast_to(array, (lax.axis_size(axis), *array.shape))
    return lax.all_to_all(sent, axis, split_axis=0, concat_axis=0, tiled=True)


def call(body, outs, name, scratch=(), scalars=0, operands=0, flops=10**8):
    specs = [pl.BlockSpec(memory_space=pltpu.SMEM)] * scalars
    specs += [pl.BlockSpec(memory_space=pltpu.VMEM)] * operands
    return pl.pallas_call(
        body,
        in_specs=specs,
        out_specs=[pl.BlockSpec(memory_space=pltpu.VMEM)] * len(outs),
        out_shape=[jax.ShapeDtypeStruct(shape, kind) for shape, kind in outs],
        scratch_shapes=list(scratch),
        compiler_params=pltpu.CompilerParams(vmem_limit_bytes=VMEM),
        cost_estimate=pl.CostEstimate(flops=flops, transcendentals=0, bytes_accessed=10**6),
        name=name,
    )


def pieces_of(width, sub=SUB):
    return [slice(j * sub, (j + 1) * sub) for j in range(width // sub)]


def times(width):
    return lax.broadcasted_iota(jnp.int32, (BLOCK, width), 0).astype(F32)


def gate_body(stream, inner, gain, v, squares, acc):
    step = pl.program_id(0)
    x = stream[...].astype(F32)
    v[...] = (inner[...].astype(F32) * x * gain[...]).astype(BF16)
    sq = x * x
    part = sq[:, :128]
    for j in range(1, x.shape[1] // 128):
        part = part + sq[:, j * 128 : (j + 1) * 128]

    @pl.when(step == 0)
    def _():
        acc[...] = part

    @pl.when(step > 0)
    def _():
        acc[...] = acc[...] + part

    @pl.when(step == pl.num_programs(0) - 1)
    def _():
        squares[...] = jnp.sum(acc[...].T, axis=0, keepdims=True)


def gated(stream, inner, gain, tile=512):
    rows, width = stream.shape
    wide = pl.BlockSpec((rows, tile), lambda i: (0, i))
    return pl.pallas_call(
        gate_body,
        grid=(width // tile,),
        in_specs=[wide, wide, pl.BlockSpec((1, tile), lambda i: (0, i))],
        out_specs=[wide, pl.BlockSpec((1, rows), lambda i: (0, 0))],
        out_shape=[
            jax.ShapeDtypeStruct((rows, width), BF16),
            jax.ShapeDtypeStruct((1, rows), F32),
        ],
        scratch_shapes=[pltpu.VMEM((rows, 128), F32)],
        compiler_params=pltpu.CompilerParams(vmem_limit_bytes=VMEM),
        name="gated",
    )(stream, inner, gain)


def tables_body(forward, taps, inner, short_outer, long_outer, decay, scale, spectrum, gate, outer):
    f_hi, f_lo = split(forward[:, :BLOCK])
    for at in pieces_of(taps.shape[1]):
        d = decay[:, at]
        spectrum[:, at] = dot(f_hi, taps[:, at]) + dot(f_lo, taps[:, at])
        time = times(SUB)
        gate[:, at] = inner[:, at].astype(F32) * short_outer[:, at].astype(F32) * jnp.exp(d * time)
        outer[:, at] = long_outer[:, at].astype(F32) * scale[:, at] * jnp.exp(-d * time)


def conv_body(
    before, here, factor, forward, back, lower, spectrum, gate, decay, total, copied, rows32
):
    fr = (forward[...] * factor[...]).astype(BF16)
    b = back[...].astype(BF16)
    for j, at in enumerate(pieces_of(here.shape[1])):
        x = dot(fr, jnp.concatenate([before[:, at], here[:, at]], axis=0))
        h = spectrum[:, at]
        x_re, x_im = x[:BLOCK], x[BLOCK:]
        h_re, h_im = h[:BLOCK], h[BLOCK:]
        y_re = (x_re * h_re - x_im * h_im).astype(BF16)
        y_im = (x_re * h_im + x_im * h_re).astype(BF16)
        conv = dot(b, jnp.concatenate([y_re, y_im], axis=0))
        result = dot(lower[...], (gate[:, at] * conv).astype(BF16))
        total[:, at] = result
        last = result[BLOCK - 1 :] * jnp.exp(decay[:, at] * (1.0 - BLOCK))
        for k in range(SUB // 128):
            row = j * (SUB // 128) + k
            rows32[row : row + 1, :] = last[:, k * 128 : (k + 1) * 128]
    state = rows32[...].astype(BF16)
    for k in range(copied.shape[0]):
        copied[k] = state


def weighted(pieces, place, rate):
    out = jnp.zeros(rate.shape, F32)
    for k in range(pieces.shape[0]):
        gap = place - 1 - k
        weight = jnp.exp(-rate * jnp.maximum(gap, 0).astype(F32))
        out = out + jnp.where(gap >= 0, weight * pieces[k].astype(F32), 0.0)
    return out


def near_body(place, pieces, rate, inside, copied):
    size = pieces.shape[0]
    inside[...] = weighted(pieces, place[0], rate[...])
    group = weighted(pieces, jnp.int32(size), rate[...]).astype(BF16)
    for k in range(copied.shape[0]):
        copied[k] = group


def finish_body(place, others, inside, rate, near_size, total, outer, decay, weights, mixed, ahead):
    near, far = place[0], place[1]
    r = rate[...]
    carry = inside[...] + jnp.exp(-r * near.astype(F32)) * weighted(
        others, far, r * near_size[0].astype(F32)
    )
    for j in range(total.shape[1] // HEAD_DIM):
        at = slice(j * HEAD_DIM, (j + 1) * HEAD_DIM)
        entering = carry[j : j + 1] * jnp.exp(-decay[:, at])
        value = (outer[:, at] * (total[:, at] + entering)).astype(BF16)
        mixed[:, at] = value
        ahead[:, at] = dot(weights[j], value).astype(BF16)


def score(query, key):
    return lax.dot_general(
        query, key, (((1,), (1,)), ((), ())), preferred_element_type=F32
    ) * HEAD_DIM ** (-0.5)


def soft(scores):
    top = jnp.max(scores, axis=1, keepdims=True)
    e = jnp.exp(scores - top)
    return e, top, jnp.sum(e, axis=1, keepdims=True)


def own_body(query, key, weights, stats):
    row = lax.broadcasted_iota(jnp.int32, (BLOCK, BLOCK), 0)
    lane = lax.broadcasted_iota(jnp.int32, (BLOCK, BLOCK), 1)
    kept = jnp.zeros((BLOCK, BLOCK), F32)
    heads = weights.shape[0]
    for j in range(heads):
        at = slice(j * HEAD_DIM, (j + 1) * HEAD_DIM)
        e, top, size = soft(jnp.where(lane <= row, score(query[:, at], key[:, at]), -1e30))
        weights[j] = e.astype(BF16)
        kept = jnp.where(lane == j, top, jnp.where(lane == heads + j, size, kept))
    stats[...] = kept


def ahead_body(query, key, weights, stats):
    lane = lax.broadcasted_iota(jnp.int32, (BLOCK, BLOCK), 1)
    kept = jnp.zeros((BLOCK, BLOCK), F32)
    heads = weights.shape[0]
    for j in range(heads):
        at = slice(j * HEAD_DIM, (j + 1) * HEAD_DIM)
        e, top, size = soft(score(query[:, at], key[:, at]))
        weights[j] = (e * (1.0 / size)).astype(BF16)
        kept = jnp.where(lane == j, top, jnp.where(lane == heads + j, size, kept))
    stats[...] = kept


def here_body(weights, mixed, here, before, partial, share):
    heads = weights.shape[0]
    lane = lax.broadcasted_iota(jnp.int32, (BLOCK, BLOCK), 1)
    kept = jnp.zeros((BLOCK, BLOCK), F32)
    for j in range(heads):
        at = slice(j * HEAD_DIM, (j + 1) * HEAD_DIM)
        top, size = here[:, j : j + 1], here[:, heads + j : heads + j + 1]
        top_b, size_b = before[:, j : j + 1], before[:, heads + j : heads + j + 1]
        top_b = jnp.where(size_b > 0.0, top_b, -1e30)
        highest = jnp.maximum(top, top_b)
        scale = jnp.exp(top - highest)
        scale_b = size_b * jnp.exp(top_b - highest)
        whole = 1.0 / (size * scale + scale_b)
        partial[:, at] = dot(weights[j], mixed[:, at]) * (scale * whole)
        kept = jnp.where(lane == j, scale_b * whole, kept)
    share[...] = kept


def join_body(partial, share, before, attended):
    for j in range(partial.shape[1] // HEAD_DIM):
        at = slice(j * HEAD_DIM, (j + 1) * HEAD_DIM)
        attended[:, at] = (
            partial[:, at] + share[:, j : j + 1] * before[:, at].astype(F32)
        ).astype(BF16)


def on_device(
    stream,
    norm_gain,
    short_outer,
    short_inner,
    short_filter,
    long_outer,
    long_inner,
    long_decay,
    query_heads,
    key_heads,
):
    rows, width = stream.shape
    heads, lanes = width // HEAD_DIM, width // 128
    decay = long_decay[None]
    scale = jnp.sqrt(-jnp.expm1(-2.0 * decay))
    rate = long_decay.reshape(lanes, 128) * rows
    near, far = lax.axis_index(NEAR), lax.axis_index(FAR)
    near_size, far_size = lax.axis_size(NEAR), lax.axis_size(FAR)
    forward, back = jnp.asarray(FORWARD), jnp.asarray(BACK)
    lower = jnp.asarray(np.tril(np.ones((rows, rows), np.float32)), BF16)
    square = ((rows, rows), F32)
    wide, wide_float = ((rows, width), BF16), ((rows, width), F32)

    query_next = shifted(query_heads, SEQ, -1)
    v, squares = gated(stream, short_inner, norm_gain[None])
    v_before = shifted(v, SEQ, 1)
    totals = jnp.sum(copies(squares, "mp"), axis=0)
    totals_before = shifted(totals, SEQ, 1)
    factor = 1.0 / jnp.sqrt(jnp.concatenate([totals_before, totals], axis=1) / D + 0.5)
    spectrum, gate, outer = call(
        tables_body,
        [((2 * rows, width), F32), wide_float, wide_float],
        "tables",
        operands=7,
    )(forward, short_filter, long_inner, short_outer, long_outer, decay, scale)
    total, state = call(
        conv_body,
        [wide_float, ((near_size, lanes, 128), BF16)],
        "conv",
        scratch=[pltpu.VMEM((lanes, 128), F32)],
        operands=9,
    )(v_before, v, factor, forward, back, lower, spectrum, gate, decay)
    pieces = lax.all_to_all(state, NEAR, 0, 0, tiled=True)
    inside, group = call(
        near_body,
        [((lanes, 128), F32), ((far_size, lanes, 128), BF16)],
        "near",
        scalars=1,
        operands=2,
    )(near[None], pieces, rate)
    others = lax.all_to_all(group, FAR, 0, 0, tiled=True)
    weights_here, stats_here = call(
        own_body, [((heads, rows, rows), BF16), square], "own", operands=2
    )(query_heads, key_heads)
    weights_next, stats_next = call(
        ahead_body, [((heads, rows, rows), BF16), square], "ahead", operands=2
    )(query_next, key_heads)
    stats_before = shifted(stats_next, SEQ, 1)
    weights_next, stats_before = lax.optimization_barrier((weights_next, stats_before))

    def finish(place, others, inside, rate, total, outer, decay, weights, mixed, ahead):
        finish_body(
            place, others, inside, rate, [jnp.int32(near_size)], total, outer, decay, weights, mixed, ahead
        )

    mixed, sent = call(finish, [wide, wide], "finish", scalars=1, operands=7)(
        jnp.stack([near, far]), others, inside, rate, total, outer, decay, weights_next
    )
    arrived = shifted(sent, SEQ, 1)
    partial, share = call(here_body, [wide_float, square], "here", operands=4)(
        weights_here, mixed, stats_here, stats_before
    )
    (attended,) = call(join_body, [wide], "join", operands=3)(partial, share, arrived)
    return (mixed, attended)


def solution(mesh):
    finer = Mesh(
        mesh.devices.reshape(8, 2, 4, 2, mesh.shape["mp"]),
        ("seq_0", "seq_1", "seq_2", "seq_3", "mp"),
    )
    placed = (
        P(SEQ, "mp"),
        P("mp"),
        P(SEQ, "mp"),
        P(SEQ, "mp"),
        P(None, "mp"),
        P(SEQ, "mp"),
        P(SEQ, "mp"),
        P("mp"),
        P(SEQ, "mp"),
        P(SEQ, "mp"),
    )
    return jax.shard_map(
        on_device,
        mesh=finer,
        in_specs=placed,
        out_specs=(P(SEQ, "mp"), P(SEQ, "mp")),
        check_vma=False,
    )
```

```python
import functools

import jax
import jax.numpy as jnp
import numpy as np
from jax import lax
from jax.experimental import pallas as pl
from jax.experimental.pallas import tpu as pltpu
from jax.sharding import Mesh
from jax.sharding import PartitionSpec as P

D = 8192
HEAD_DIM = 128
BLOCK = 128
SEQ = ("seq_0", "seq_1", "seq_2", "seq_3")
NEAR = ("seq_2", "seq_3")
FAR = ("seq_0", "seq_1")
F32 = jnp.float32
BF16 = jnp.bfloat16
SUB = 256
VMEM = 8 * 2**20


def dft_matrices():
    n = 2 * BLOCK
    k = np.arange(BLOCK, dtype=np.float64)[:, None]
    t = np.arange(n, dtype=np.float64)[None, :]
    angle = np.pi * (2 * k + 1) * t / n
    forward = np.concatenate([np.cos(angle), -np.sin(angle)], axis=0)
    back = np.concatenate([np.cos(angle), -np.sin(angle)], axis=0).T[BLOCK:] * (2.0 / n)
    return forward.astype(np.float32), back.astype(np.float32)


FORWARD, BACK = dft_matrices()


def split(value):
    high = value.astype(BF16)
    return high, (value - high.astype(F32)).astype(BF16)


def dot(a, b):
    return jnp.dot(a, b, preferred_element_type=F32)


def shifted(block, axis, distance):
    size = lax.axis_size(axis)
    return lax.ppermute(block, axis, [(i, i + distance) for i in range(size) if 0 <= i + distance < size])


def swapped(block):
    sides = lax.axis_size("mp")
    return lax.ppermute(block, "mp", [(m, sides - 1 - m) for m in range(sides)])


def call(body, outs, name, scratch=(), scalars=0, operands=0, flops=10**8):
    specs = [pl.BlockSpec(memory_space=pltpu.SMEM)] * scalars
    specs += [pl.BlockSpec(memory_space=pltpu.VMEM)] * operands
    return pl.pallas_call(
        body,
        in_specs=specs,
        out_specs=[pl.BlockSpec(memory_space=pltpu.VMEM)] * len(outs),
        out_shape=[jax.ShapeDtypeStruct(shape, kind) for shape, kind in outs],
        scratch_shapes=list(scratch),
        compiler_params=pltpu.CompilerParams(vmem_limit_bytes=VMEM),
        cost_estimate=pl.CostEstimate(flops=flops, transcendentals=0, bytes_accessed=10**6),
        name=name,
    )


def pieces_of(width, sub=SUB):
    return [slice(j * sub, (j + 1) * sub) for j in range(width // sub)]


def times(width):
    return lax.broadcasted_iota(jnp.int32, (BLOCK, width), 0).astype(F32)


def squares_body(stream, squares):
    acc = jnp.zeros((stream.shape[0], 128), F32)
    for at in pieces_of(stream.shape[1], 128):
        x = stream[:, at].astype(F32)
        acc = acc + x * x
    squares[...] = jnp.sum(acc.T, axis=0, keepdims=True)


def gate_body(stream, inner, gain, v, sent):
    for at in pieces_of(stream.shape[1], 128):
        value = inner[:, at].astype(F32) * stream[:, at].astype(F32) * gain[:, at]
        v[:, at] = value.astype(BF16)
        sent[:, at] = value.astype(BF16)


def label_body(squares, beside, sent, total, out):
    value = squares[...] + beside[...]
    total[...] = value
    first = lax.broadcasted_iota(jnp.int32, (16, 128), 0) == 0
    for k in range(3):
        col = slice(k * 128, (k + 1) * 128)
        term = value.astype(BF16).astype(F32)
        value = value - term
        out[:, col] = jnp.where(first, term, sent[:, col].astype(F32)).astype(BF16)


def label(squares, beside, sent):
    rows, width = sent.shape
    part = pl.BlockSpec((16, 3 * 128), lambda i: (0, 0))
    row = pl.BlockSpec((1, rows), lambda i: (0, 0))
    return pl.pallas_call(
        label_body,
        grid=(1,),
        in_specs=[row, row, part],
        out_specs=[row, part],
        out_shape=[jax.ShapeDtypeStruct((1, rows), F32), jax.ShapeDtypeStruct((rows, width), BF16)],
        input_output_aliases={2: 1},
        compiler_params=pltpu.CompilerParams(vmem_limit_bytes=VMEM),
        name="label",
    )(squares, beside, sent)


def tables_body(forward, taps, inner, short_outer, decay, spectrum, gate):
    f_hi, f_lo = split(forward[:, :BLOCK])
    for at in pieces_of(taps.shape[1]):
        d = decay[:, at]
        spectrum[:, at] = dot(f_hi, taps[:, at]) + dot(f_lo, taps[:, at])
        time = times(SUB)
        gate[:, at] = inner[:, at].astype(F32) * short_outer[:, at].astype(F32) * jnp.exp(d * time)


def conv_body(
    before,
    here,
    squares,
    forward,
    back,
    lower,
    spectrum,
    gate,
    decay,
    summed,
    copied,
    rows32,
):
    carried = before[:16, : 3 * 128].astype(F32)
    earlier = (carried[:1, :128] + carried[:1, 128:256]) + carried[:1, 256:]
    sums = jnp.concatenate([earlier, squares[...]], axis=1)
    column = lax.broadcasted_iota(jnp.int32, (1, 2 * BLOCK), 1)
    factor = jnp.where(column == 0, 0.0, 1.0 / jnp.sqrt(sums / D + 0.5))
    fr = (forward[...] * factor).astype(BF16)
    b = back[...].astype(BF16)
    for j, at in enumerate(pieces_of(here.shape[1])):
        x = dot(fr, jnp.concatenate([before[:, at], here[:, at]], axis=0))
        h = spectrum[:, at]
        x_re, x_im = x[:BLOCK], x[BLOCK:]
        h_re, h_im = h[:BLOCK], h[BLOCK:]
        y_re = (x_re * h_re - x_im * h_im).astype(BF16)
        y_im = (x_re * h_im + x_im * h_re).astype(BF16)
        conv = dot(b, jnp.concatenate([y_re, y_im], axis=0))
        z = (gate[:, at] * conv).astype(BF16)
        summed[:, at] = z
        result = dot(lower[...], z)
        last = result[BLOCK - 1 :] * jnp.exp(decay[:, at] * (1.0 - BLOCK))
        for k in range(SUB // 128):
            row = j * (SUB // 128) + k
            rows32[row : row + 1, :] = last[:, k * 128 : (k + 1) * 128]
    state = rows32[...].astype(BF16)
    for k in range(copied.shape[0]):
        copied[k] = state


def weighted(pieces, place, rate):
    out = jnp.zeros(rate.shape, F32)
    for k in range(pieces.shape[0]):
        gap = place - 1 - k
        weight = jnp.exp(-rate * jnp.maximum(gap, 0).astype(F32))
        out = out + jnp.where(gap >= 0, weight * pieces[k].astype(F32), 0.0)
    return out


def near_body(place, pieces, rate, inside, copied):
    size = pieces.shape[0]
    inside[...] = weighted(pieces, place[0], rate[...])
    group = weighted(pieces, jnp.int32(size), rate[...]).astype(BF16)
    for k in range(copied.shape[0]):
        copied[k] = group


def finish_body(near_size, place, others, inside, rate, summed, lower, long_outer, decay, scale, weights, mixed, ahead):
    near, far = place[0], place[1]
    r = rate[...]
    carry = inside[...] + jnp.exp(-r * near.astype(F32)) * weighted(others, far, r * near_size)
    time = times(HEAD_DIM)
    for j in range(summed.shape[1] // HEAD_DIM):
        at = slice(j * HEAD_DIM, (j + 1) * HEAD_DIM)
        d = decay[:, at]
        entering = carry[j : j + 1] * jnp.exp(-d)
        outer = long_outer[:, at].astype(F32) * (jnp.exp(-d * time) * scale[:, at])
        value = (outer * (dot(lower[...], summed[:, at]) + entering)).astype(BF16)
        mixed[:, at] = value
        ahead[:, at] = dot(weights[j], value).astype(BF16)


def score(query, key):
    return lax.dot_general(
        query, key, (((1,), (1,)), ((), ())), preferred_element_type=F32
    ) * HEAD_DIM ** (-0.5)


def soft(scores):
    top = jnp.max(scores, axis=1, keepdims=True)
    e = jnp.exp(scores - top)
    return e, top, jnp.sum(e, axis=1, keepdims=True)


def own_body(query, key, weights, stats):
    row = lax.broadcasted_iota(jnp.int32, (BLOCK, BLOCK), 0)
    lane = lax.broadcasted_iota(jnp.int32, (BLOCK, BLOCK), 1)
    tops = jnp.zeros((BLOCK, BLOCK), F32)
    sizes = jnp.zeros((BLOCK, BLOCK), F32)
    for j in range(weights.shape[0]):
        at = slice(j * HEAD_DIM, (j + 1) * HEAD_DIM)
        e, top, size = soft(jnp.where(lane <= row, score(query[:, at], key[:, at]), -1e30))
        weights[j] = e.astype(BF16)
        tops = jnp.where(lane == j, top, tops)
        sizes = jnp.where(lane == j + BLOCK // 2, size, sizes)
    stats[...] = jnp.where(lane < BLOCK // 2, tops, sizes)


def ahead_body(query, key, weights, stats):
    lane = lax.broadcasted_iota(jnp.int32, (BLOCK, BLOCK), 1)
    tops = jnp.zeros((BLOCK, BLOCK), F32)
    sizes = jnp.zeros((BLOCK, BLOCK), F32)
    for j in range(weights.shape[0]):
        at = slice(j * HEAD_DIM, (j + 1) * HEAD_DIM)
        e, top, size = soft(score(query[:, at], key[:, at]))
        weights[j] = (e * (1.0 / size)).astype(BF16)
        tops = jnp.where(lane == j, top, tops)
        sizes = jnp.where(lane == j + BLOCK // 2, size, sizes)
    stats[...] = jnp.where(lane < BLOCK // 2, tops, sizes)


def here_body(weights, mixed, here, before, partial, share):
    top, size = here[...], pltpu.roll(here[...], BLOCK // 2, 1)
    size_b = pltpu.roll(before[...], BLOCK // 2, 1)
    top_b = jnp.where(size_b > 0.0, before[...], -1e30)
    highest = jnp.maximum(top, top_b)
    scale = jnp.exp(top - highest)
    scale_b = size_b * jnp.exp(top_b - highest)
    whole = 1.0 / (size * scale + scale_b)
    own = scale * whole
    share[...] = scale_b * whole
    for j in range(weights.shape[0]):
        at = slice(j * HEAD_DIM, (j + 1) * HEAD_DIM)
        partial[:, at] = dot(weights[j], mixed[:, at]) * own[:, j : j + 1]


def join_body(partial, share, before, attended):
    for j in range(partial.shape[1] // HEAD_DIM):
        at = slice(j * HEAD_DIM, (j + 1) * HEAD_DIM)
        attended[:, at] = (
            partial[:, at] + share[:, j : j + 1] * before[:, at].astype(F32)
        ).astype(BF16)


def on_device(
    stream,
    norm_gain,
    short_outer,
    short_inner,
    short_filter,
    long_outer,
    long_inner,
    long_decay,
    query_heads,
    key_heads,
):
    rows, width = stream.shape
    heads, lanes = width // HEAD_DIM, width // 128
    decay = long_decay[None]
    scale = jnp.sqrt(-jnp.expm1(-2.0 * decay))
    rate = long_decay.reshape(lanes, 128) * rows
    near, far = lax.axis_index(NEAR), lax.axis_index(FAR)
    near_size, far_size = lax.axis_size(NEAR), lax.axis_size(FAR)
    forward, back = jnp.asarray(FORWARD), jnp.asarray(BACK)
    lower = jnp.asarray(np.tril(np.ones((rows, rows), np.float32)), BF16)
    square = ((rows, rows), F32)
    wide, wide_float = ((rows, width), BF16), ((rows, width), F32)

    (squares,) = call(squares_body, [((1, rows), F32)], "squares", operands=1)(stream)
    beside = swapped(squares)
    v, sent = call(gate_body, [wide, wide], "gate", operands=3)(stream, short_inner, norm_gain[None])
    total, sent = label(squares, beside, sent)
    v_before = shifted(sent, SEQ, 1)
    queries, total = lax.optimization_barrier((query_heads, total))
    query_next = shifted(queries, SEQ, -1)
    spectrum, gate = call(
        tables_body, [((2 * rows, width), F32), wide_float], "tables", operands=5
    )(forward, short_filter, long_inner, short_outer, decay)
    weights_here, stats_here = call(
        own_body, [((heads, rows, rows), BF16), square], "own", operands=2
    )(query_heads, key_heads)
    v_before, stats_here = lax.optimization_barrier((v_before, stats_here))
    summed, state = call(
        conv_body,
        [wide, ((near_size, lanes, 128), BF16)],
        "conv",
        scratch=[pltpu.VMEM((lanes, 128), F32)],
        operands=9,
    )(v_before, v, total, forward, back, lower, spectrum, gate, decay)
    pieces = lax.all_to_all(state, NEAR, 0, 0, tiled=True)
    weights_next, stats_next = call(
        ahead_body, [((heads, rows, rows), BF16), square], "ahead", operands=2
    )(query_next, key_heads)
    pieces, stats_next = lax.optimization_barrier((pieces, stats_next))
    stats_before = shifted(stats_next, SEQ, 1)
    inside, group = call(
        near_body,
        [((lanes, 128), F32), ((far_size, lanes, 128), BF16)],
        "near",
        scalars=1,
        operands=2,
    )(near[None], pieces, rate)
    others = lax.all_to_all(group, FAR, 0, 0, tiled=True)
    others, stats_before = lax.optimization_barrier((others, stats_before))
    mixed, sent = call(
        functools.partial(finish_body, float(near_size)), [wide, wide], "finish", scalars=1, operands=9
    )(
        jnp.stack([near, far]),
        others,
        inside,
        rate,
        summed,
        lower,
        long_outer,
        decay,
        scale,
        weights_next,
    )
    arrived = shifted(sent, SEQ, 1)
    partial, share = call(here_body, [wide_float, square], "here", operands=4)(
        weights_here, mixed, stats_here, stats_before
    )
    (attended,) = call(join_body, [wide], "join", operands=3)(partial, share, arrived)
    return (mixed, attended)


def solution(mesh):
    finer = Mesh(
        mesh.devices.reshape(8, 2, 4, 2, mesh.shape["mp"]),
        ("seq_0", "seq_1", "seq_2", "seq_3", "mp"),
    )
    placed = (
        P(SEQ, "mp"),
        P("mp"),
        P(SEQ, "mp"),
        P(SEQ, "mp"),
        P(None, "mp"),
        P(SEQ, "mp"),
        P(SEQ, "mp"),
        P("mp"),
        P(SEQ, "mp"),
        P(SEQ, "mp"),
    )
    return jax.shard_map(
        on_device,
        mesh=finer,
        in_specs=placed,
        out_specs=(P(SEQ, "mp"), P(SEQ, "mp")),
        check_vma=False,
    )
```

```python
import functools

import jax
import jax.numpy as jnp
import numpy as np
from jax import lax
from jax.experimental import pallas as pl
from jax.experimental.pallas import tpu as pltpu
from jax.sharding import Mesh
from jax.sharding import PartitionSpec as P

D = 8192
HEAD_DIM = 128
BLOCK = 128
SEQ = ("seq_0", "seq_1", "seq_2", "seq_3")
NEAR = ("seq_2", "seq_3")
FAR = ("seq_0", "seq_1")
F32 = jnp.float32
BF16 = jnp.bfloat16
SUB = 256
PARTS = 2
CHUNKS = 4
VMEM = 8 * 2**20


def dft_matrices():
    n = 2 * BLOCK
    k = np.arange(BLOCK, dtype=np.float64)[:, None]
    t = np.arange(n, dtype=np.float64)[None, :]
    angle = np.pi * (2 * k + 1) * t / n
    forward = np.concatenate([np.cos(angle), -np.sin(angle)], axis=0)
    back = np.concatenate([np.cos(angle), -np.sin(angle)], axis=0).T[BLOCK:] * (2.0 / n)
    return forward.astype(np.float32), back.astype(np.float32)


FORWARD, BACK = dft_matrices()


def split(value):
    high = value.astype(BF16)
    return high, (value - high.astype(F32)).astype(BF16)


def dot(a, b):
    return jnp.dot(a, b, preferred_element_type=F32)


def shifted(block, axis, distance):
    size = lax.axis_size(axis)
    return lax.ppermute(block, axis, [(i, i + distance) for i in range(size) if 0 <= i + distance < size])


def swapped(block):
    sides = lax.axis_size("mp")
    return lax.ppermute(block, "mp", [(m, sides - 1 - m) for m in range(sides)])


def call(body, outs, scratch=(), scalars=0, operands=0, flops=10**8, outside=(), kept=()):
    specs = [pl.BlockSpec(memory_space=pltpu.SMEM)] * scalars
    specs += [pl.BlockSpec(memory_space=pltpu.VMEM)] * operands
    for k in outside:
        specs[k] = pl.BlockSpec(memory_space=pltpu.HBM)
    return pl.pallas_call(
        body,
        in_specs=specs,
        out_specs=[
            pl.BlockSpec(memory_space=pltpu.HBM if k in kept else pltpu.VMEM)
            for k in range(len(outs))
        ],
        out_shape=[
            pltpu.HBM(shape, kind) if k in kept else jax.ShapeDtypeStruct(shape, kind)
            for k, (shape, kind) in enumerate(outs)
        ],
        scratch_shapes=list(scratch),
        compiler_params=pltpu.CompilerParams(vmem_limit_bytes=VMEM),
        cost_estimate=pl.CostEstimate(flops=flops, transcendentals=0, bytes_accessed=10**6),
    )


def in_hbm(array):
    return pltpu.with_memory_space_constraint(array, pltpu.HBM)


def pieces_of(width, sub=SUB):
    return [slice(j * sub, (j + 1) * sub) for j in range(width // sub)]


def times(width):
    return lax.broadcasted_iota(jnp.int32, (BLOCK, width), 0).astype(F32)


def squares_body(stream, squares):
    acc = jnp.zeros((stream.shape[0], 128), F32)
    for at in pieces_of(stream.shape[1], 128):
        x = stream[:, at].astype(F32)
        acc = acc + x * x
    squares[...] = jnp.sum(acc.T, axis=0, keepdims=True)


def gate_body(stream, inner, gain, v, *sent):
    share = stream.shape[1] // len(sent)
    for at in pieces_of(stream.shape[1], 128):
        value = inner[:, at].astype(F32) * stream[:, at].astype(F32) * gain[:, at]
        v[:, at] = value.astype(BF16)
        start = at.start % share
        sent[at.start // share][:, start : start + 128] = value.astype(BF16)


def label_body(squares, beside, sent, total, out):
    value = squares[...] + beside[...]
    total[...] = value
    first = lax.broadcasted_iota(jnp.int32, (16, 128), 0) == 0
    for k in range(3):
        col = slice(k * 128, (k + 1) * 128)
        term = value.astype(BF16).astype(F32)
        value = value - term
        out[:, col] = jnp.where(first, term, sent[:, col].astype(F32)).astype(BF16)


def label(squares, beside, sent):
    rows, width = sent.shape
    part = pl.BlockSpec((16, 3 * 128), lambda i: (0, 0))
    row = pl.BlockSpec((1, rows), lambda i: (0, 0))
    return pl.pallas_call(
        label_body,
        grid=(1,),
        in_specs=[row, row, part],
        out_specs=[row, part],
        out_shape=[jax.ShapeDtypeStruct((1, rows), F32), jax.ShapeDtypeStruct((rows, width), BF16)],
        input_output_aliases={2: 1},
        compiler_params=pltpu.CompilerParams(vmem_limit_bytes=VMEM),
        name="label",
    )(squares, beside, sent)


def tables_body(forward, taps, inner, short_outer, decay, spectrum, gate):
    f_hi, f_lo = split(forward[:, :BLOCK])
    for at in pieces_of(taps.shape[1]):
        d = decay[:, at]
        spectrum[:, at] = dot(f_hi, taps[:, at]) + dot(f_lo, taps[:, at])
        time = times(SUB)
        gate[:, at] = inner[:, at].astype(F32) * short_outer[:, at].astype(F32) * jnp.exp(d * time)


def conv_first(
    before, here, squares, forward, back, lower, spectrum, gate, decay, far, state, matrix, summed, sems
):
    carried = before[:16, : 3 * 128].astype(F32)
    earlier = (carried[:1, :128] + carried[:1, 128:256]) + carried[:1, 256:]
    sums = jnp.concatenate([earlier, squares[...]], axis=1)
    column = lax.broadcasted_iota(jnp.int32, (1, 2 * BLOCK), 1)
    factor = jnp.where(column == 0, 0.0, 1.0 / jnp.sqrt(sums / D + 0.5))
    matrix[...] = (forward[...] * factor).astype(BF16)
    conv_body(0, before, here, matrix, back, lower, spectrum, gate, decay, far, state, summed, sems)


def conv_last(
    start, before, here, matrix, back, lower, spectrum, gate, decay, earlier, far, copied, rows, summed, sems
):
    conv_body(start, before, here, matrix, back, lower, spectrum, gate, decay, far, rows, summed, sems)
    state = jnp.concatenate([earlier[...], rows[...]], axis=0).astype(BF16)
    for k in range(copied.shape[0]):
        copied[k] = state


def conv_body(
    start, before, here, matrix, back, lower, spectrum, gate, decay, far, state, summed, sems
):
    b = back[...].astype(BF16)
    leaving = []
    width = before.shape[1] // CHUNKS
    for j, to in enumerate(pieces_of(before.shape[1])):
        at = slice(start + to.start, start + to.stop)
        x = dot(matrix[...], jnp.concatenate([before[:, to], here[:, at]], axis=0))
        h = spectrum[:, at]
        x_re, x_im = x[:BLOCK], x[BLOCK:]
        h_re, h_im = h[:BLOCK], h[BLOCK:]
        y_re = (x_re * h_re - x_im * h_im).astype(BF16)
        y_im = (x_re * h_im + x_im * h_re).astype(BF16)
        conv = dot(b, jnp.concatenate([y_re, y_im], axis=0))
        z = (gate[:, at] * conv).astype(BF16)
        summed[:, to] = z
        result = dot(lower[...], z)
        last = result[BLOCK - 1 :] * jnp.exp(decay[:, at] * (1.0 - BLOCK))
        for k in range(SUB // 128):
            row = j * (SUB // 128) + k
            state[row : row + 1, :] = last[:, k * 128 : (k + 1) * 128]
        if to.stop % width == 0:
            chunk = to.stop // width - 1
            at = pl.ds(chunk * width, width)
            leaving.append(pltpu.make_async_copy(summed.at[:, at], far.at[:, at], sems.at[chunk]))
            leaving[-1].start()
    for copy in leaving:
        copy.wait()


def weighted(pieces, place, rate, some=slice(None)):
    out = jnp.zeros(rate.shape, F32)
    for k in range(pieces.shape[0]):
        gap = place - 1 - k
        weight = jnp.exp(-rate * jnp.maximum(gap, 0).astype(F32))
        out = out + jnp.where(gap >= 0, weight * pieces[k, some].astype(F32), 0.0)
    return out


def near_body(place, pieces, rate, inside, copied):
    size, r = pieces.shape[0], rate[...]
    inside[...] = weighted(pieces, place[0], r)
    group = weighted(pieces, jnp.int32(size), r).astype(BF16)
    for k in range(copied.shape[0]):
        copied[k] = group


def finish_body(
    part,
    near_size,
    place,
    others,
    inside,
    rate,
    summed_far,
    lower,
    outer_far,
    decay,
    scale,
    weights,
    mixed,
    ahead,
    summed,
    long_outer,
    summed_sems,
    outer_sems,
):
    width = long_outer.shape[1] // CHUNKS
    summed_in = fetches(summed_far, summed, summed_sems, 0, width)
    outer_in = fetches(outer_far, long_outer, outer_sems, part * long_outer.shape[1], width)
    near, far = place[0], place[1]
    lanes = others.shape[1] // PARTS
    some = slice(part * lanes, (part + 1) * lanes)
    r = rate[some]
    carry = inside[some] + jnp.exp(-r * near.astype(F32)) * weighted(
        others, far, r * near_size, some
    )
    time = times(width)
    group = width // HEAD_DIM
    for k in range(CHUNKS):
        to = slice(k * width, (k + 1) * width)
        at = slice(part * lanes * HEAD_DIM + to.start, part * lanes * HEAD_DIM + to.stop)
        d = decay[:, at]
        entering = jnp.concatenate(
            [carry[j : j + 1] for j in range(k * group, (k + 1) * group)], axis=1
        ) * jnp.exp(-d)
        factor = jnp.exp(-d * time) * scale[:, at]
        summed_in[k].wait()
        base = dot(lower[...], summed[:, to]) + entering
        outer_in[k].wait()
        mixed[:, to] = (long_outer[:, to].astype(F32) * factor * base).astype(BF16)
    for j in range(lanes):
        to = slice(j * HEAD_DIM, (j + 1) * HEAD_DIM)
        ahead[:, to] = dot(weights[part * lanes + j], mixed[:, to]).astype(BF16)


def score(query, key):
    return lax.dot_general(
        query, key, (((1,), (1,)), ((), ())), preferred_element_type=F32
    ) * HEAD_DIM ** (-0.5)


def soft(scores):
    top = jnp.max(scores, axis=1, keepdims=True)
    e = jnp.exp(scores - top)
    return e, top, jnp.sum(e, axis=1, keepdims=True)


def fetches(source, target, sems, first, width):
    copies = []
    for k in range(target.shape[1] // width):
        to = pl.ds(k * width, width)
        at = pl.ds(first + k * width, width)
        copies.append(pltpu.make_async_copy(source.at[:, at], target.at[:, to], sems.at[k]))
    for copy in copies:
        copy.start()
    return copies


def own_body(query_far, key_far, weights, stats, query, key, query_sems, key_sems):
    width = key.shape[1] // CHUNKS
    arriving = [
        pair
        for pair in zip(
            fetches(query_far, query, query_sems, 0, width),
            fetches(key_far, key, key_sems, 0, width),
        )
    ]
    row = lax.broadcasted_iota(jnp.int32, (BLOCK, BLOCK), 0)
    lane = lax.broadcasted_iota(jnp.int32, (BLOCK, BLOCK), 1)
    tops = jnp.zeros((BLOCK, BLOCK), F32)
    sizes = jnp.zeros((BLOCK, BLOCK), F32)
    for j in range(weights.shape[0]):
        at = slice(j * HEAD_DIM, (j + 1) * HEAD_DIM)
        if at.start % width == 0:
            for copy in arriving[at.start // width]:
                copy.wait()
        e, top, size = soft(jnp.where(lane <= row, score(query[:, at], key[:, at]), -1e30))
        weights[j] = e.astype(BF16)
        tops = jnp.where(lane == j, top, tops)
        sizes = jnp.where(lane == j + BLOCK // 2, size, sizes)
    stats[...] = jnp.where(lane < BLOCK // 2, tops, sizes)


def ahead_body(query, key_far, weights, stats, key, sems):
    width = key.shape[1] // CHUNKS
    arriving = fetches(key_far, key, sems, 0, width)
    lane = lax.broadcasted_iota(jnp.int32, (BLOCK, BLOCK), 1)
    tops = jnp.zeros((BLOCK, BLOCK), F32)
    sizes = jnp.zeros((BLOCK, BLOCK), F32)
    for j in range(weights.shape[0]):
        at = slice(j * HEAD_DIM, (j + 1) * HEAD_DIM)
        if at.start % width == 0:
            arriving[at.start // width].wait()
        e, top, size = soft(score(query[:, at], key[:, at]))
        weights[j] = (e * (1.0 / size)).astype(BF16)
        tops = jnp.where(lane == j, top, tops)
        sizes = jnp.where(lane == j + BLOCK // 2, size, sizes)
    stats[...] = jnp.where(lane < BLOCK // 2, tops, sizes)


def here_body(part, weights, mixed, partial):
    heads = partial.shape[1] // HEAD_DIM
    for j in range(heads):
        at = slice(j * HEAD_DIM, (j + 1) * HEAD_DIM)
        partial[:, at] = dot(weights[part * heads + j], mixed[:, at])


def join_body(part, partial, before, stats_here, stats_before, *rest):
    attended = rest[-1]
    top, size = stats_here[...], pltpu.roll(stats_here[...], BLOCK // 2, 1)
    size_b = pltpu.roll(stats_before[...], BLOCK // 2, 1)
    top_b = jnp.where(size_b > 0.0, stats_before[...], -1e30)
    highest = jnp.maximum(top, top_b)
    scale = jnp.exp(top - highest)
    scale_b = size_b * jnp.exp(top_b - highest)
    whole = 1.0 / (size * scale + scale_b)
    own, share = scale * whole, scale_b * whole
    heads = partial.shape[1] // HEAD_DIM
    for j in range(heads):
        at = slice(j * HEAD_DIM, (j + 1) * HEAD_DIM)
        head = part * heads + j
        attended[:, at] = (
            partial[:, at] * own[:, head : head + 1]
            + share[:, head : head + 1] * before[:, at].astype(F32)
        ).astype(BF16)


def copy_body(block, *rest):
    rest[-1][...] = block[...]


def into(body, part, operands, whole, width):
    rows = operands[0].shape[0]
    share = width // PARTS
    specs = [pl.BlockSpec(x.shape, lambda i: (0, 0)) for x in operands]
    aliases = {}
    if whole is not None:
        specs.append(pl.BlockSpec(memory_space=pl.ANY))
        aliases = {len(operands): 0}
        operands = (*operands, whole)
    return pl.pallas_call(
        body,
        grid=(1,),
        in_specs=specs,
        out_specs=pl.BlockSpec((rows, share), lambda i: (0, part)),
        out_shape=jax.ShapeDtypeStruct((rows, width), BF16),
        input_output_aliases=aliases,
        compiler_params=pltpu.CompilerParams(vmem_limit_bytes=VMEM),
    )(*operands)


def on_device(
    stream,
    norm_gain,
    short_outer,
    short_inner,
    short_filter,
    long_outer,
    long_inner,
    long_decay,
    query_heads,
    key_heads,
):
    rows, width = stream.shape
    heads, lanes = width // HEAD_DIM, width // 128
    decay = long_decay[None]
    scale = jnp.sqrt(-jnp.expm1(-2.0 * decay))
    rate = long_decay.reshape(lanes, 128) * rows
    near, far = lax.axis_index(NEAR), lax.axis_index(FAR)
    near_size, far_size = lax.axis_size(NEAR), lax.axis_size(FAR)
    forward, back = jnp.asarray(FORWARD), jnp.asarray(BACK)
    lower = jnp.asarray(np.tril(np.ones((rows, rows), np.float32)), BF16)
    square = ((rows, rows), F32)
    wide, wide_float = ((rows, width), BF16), ((rows, width), F32)

    half = ((rows, width // PARTS), BF16)
    some = lanes // PARTS
    (squares,) = call(squares_body, [((1, rows), F32)], operands=1)(stream)
    beside = swapped(squares)
    v, *sent = call(gate_body, [wide] + [half] * PARTS, operands=3)(
        stream, short_inner, norm_gain[None]
    )
    total, sent[0] = label(squares, beside, sent[0])
    v_before = []
    for part in range(PARTS):
        v_before.append(shifted(sent[part], SEQ, 1))
    queries, total = lax.optimization_barrier((query_heads, total))
    query_next = shifted(queries, SEQ, -1)
    spectrum, gate = call(
        tables_body, [((2 * rows, width), F32), wide_float], operands=5
    )(forward, short_filter, long_inner, short_outer, decay)
    some_state = ((some, 128), F32)
    leaving = [pltpu.VMEM((rows, width // PARTS), BF16), pltpu.SemaphoreType.DMA((CHUNKS,))]
    first, early, matrix = call(
        conv_first, [half, some_state, ((2 * rows, 2 * rows), BF16)], leaving, operands=9, kept=(0,)
    )(v_before[0], v, total, forward, back, lower, spectrum, gate, decay)
    last, state = call(
        functools.partial(conv_last, width // PARTS),
        [half, ((near_size, lanes, 128), BF16)],
        [pltpu.VMEM((some, 128), F32), *leaving],
        operands=9,
        kept=(0,),
    )(v_before[1], v, matrix, back, lower, spectrum, gate, decay, early)
    summed = [first, last]
    pieces = lax.all_to_all(state, NEAR, 0, 0, tiled=True)
    weights_here, stats_here = call(
        own_body,
        [((heads, rows, rows), BF16), square],
        [pltpu.VMEM((rows, width), BF16)] * 2 + [pltpu.SemaphoreType.DMA((CHUNKS,))] * 2,
        operands=2,
        outside=(0, 1),
    )(in_hbm(query_heads), in_hbm(key_heads))
    pieces, stats_here = lax.optimization_barrier((pieces, stats_here))
    inside, group = call(
        near_body, [((lanes, 128), F32), ((far_size, lanes, 128), BF16)], scalars=1, operands=2
    )(near[None], pieces, rate)
    others = lax.all_to_all(group, FAR, 0, 0, tiled=True)
    query_next, keys, inside = lax.optimization_barrier((query_next, key_heads, inside))
    weights_next, stats_next = call(
        ahead_body,
        [((heads, rows, rows), BF16), square],
        [pltpu.VMEM((rows, width), BF16), pltpu.SemaphoreType.DMA((CHUNKS,))],
        operands=2,
        outside=(1,),
    )(query_next, in_hbm(keys))
    stats_before = shifted(stats_next, SEQ, 1)
    mixed, arrived = [], []
    for part in range(PARTS):
        block, ready = call(
            functools.partial(finish_body, part, float(near_size)),
            [half, half],
            [pltpu.VMEM((rows, width // PARTS), BF16)] * 2
            + [pltpu.SemaphoreType.DMA((CHUNKS,))] * 2,
            scalars=1,
            operands=9,
            outside=(4, 6),
        )(
            jnp.stack([near, far]),
            others,
            inside,
            rate,
            in_hbm(summed[part]),
            lower,
            in_hbm(long_outer),
            decay,
            scale,
            weights_next,
        )
        mixed.append(block)
        arrived.append(shifted(ready, SEQ, 1))
    attended = values = None
    for part in range(PARTS):
        (partial,) = call(
            functools.partial(here_body, part), [((rows, width // PARTS), F32)], operands=2
        )(weights_here, mixed[part])
        values = into(copy_body, part, (mixed[part],), values, width)
        attended = into(
            functools.partial(join_body, part),
            part,
            (partial, arrived[part], stats_here, stats_before),
            attended,
            width,
        )
    return (values, attended)


def solution(mesh):
    finer = Mesh(
        mesh.devices.reshape(8, 2, 4, 2, mesh.shape["mp"]),
        ("seq_0", "seq_1", "seq_2", "seq_3", "mp"),
    )
    placed = (
        P(SEQ, "mp"),
        P("mp"),
        P(SEQ, "mp"),
        P(SEQ, "mp"),
        P(None, "mp"),
        P(SEQ, "mp"),
        P(SEQ, "mp"),
        P("mp"),
        P(SEQ, "mp"),
        P(SEQ, "mp"),
    )
    return jax.shard_map(
        on_device,
        mesh=finer,
        in_specs=placed,
        out_specs=(P(SEQ, "mp"), P(SEQ, "mp")),
        check_vma=False,
    )
```

```python
import functools

import jax
import jax.numpy as jnp
import numpy as np
from jax import lax
from jax.experimental import pallas as pl
from jax.experimental.pallas import tpu as pltpu
from jax.sharding import Mesh
from jax.sharding import PartitionSpec as P

D = 8192
HEAD_DIM = 128
BLOCK = 128
SEQ = ("seq_0", "seq_1", "seq_2", "seq_3")
NEAR = ("seq_2", "seq_3")
FAR = ("seq_0", "seq_1")
F32 = jnp.float32
BF16 = jnp.bfloat16
SUB = 256
PIECE = 512
TAIL = (3072, 1024)
EARLY = 1024
MIDDLE = 2048
VMEM = 8 * 2**20


def dft_matrices():
    n = 2 * BLOCK
    k = np.arange(BLOCK, dtype=np.float64)[:, None]
    t = np.arange(n, dtype=np.float64)[None, :]
    angle = np.pi * (2 * k + 1) * t / n
    forward = np.concatenate([np.cos(angle), -np.sin(angle)], axis=0)
    back = np.concatenate([np.cos(angle), -np.sin(angle)], axis=0).T[BLOCK:] * (2.0 / n)
    return forward.astype(np.float32), back.astype(np.float32)


FORWARD, BACK = dft_matrices()


def split(value):
    high = value.astype(BF16)
    return high, (value - high.astype(F32)).astype(BF16)


def dot(a, b):
    return jnp.dot(a, b, preferred_element_type=F32)


def shifted(block, axis, distance):
    size = lax.axis_size(axis)
    return lax.ppermute(block, axis, [(i, i + distance) for i in range(size) if 0 <= i + distance < size])


def swapped(block):
    sides = lax.axis_size("mp")
    return lax.ppermute(block, "mp", [(m, sides - 1 - m) for m in range(sides)])


def call(body, outs, scratch=(), scalars=0, operands=0, flops=10**8, outside=(), kept=(), aliases={}):
    specs = [pl.BlockSpec(memory_space=pltpu.SMEM)] * scalars
    specs += [pl.BlockSpec(memory_space=pltpu.VMEM)] * operands
    for k in outside:
        specs[k] = pl.BlockSpec(memory_space=pltpu.HBM)
    return pl.pallas_call(
        body,
        in_specs=specs,
        out_specs=[
            pl.BlockSpec(memory_space=pltpu.HBM if k in kept else pltpu.VMEM)
            for k in range(len(outs))
        ],
        out_shape=[
            pltpu.HBM(shape, kind) if k in kept else jax.ShapeDtypeStruct(shape, kind)
            for k, (shape, kind) in enumerate(outs)
        ],
        scratch_shapes=list(scratch),
        input_output_aliases=aliases,
        compiler_params=pltpu.CompilerParams(vmem_limit_bytes=VMEM),
        cost_estimate=pl.CostEstimate(flops=flops, transcendentals=0, bytes_accessed=10**6),
    )


def in_hbm(array):
    return pltpu.with_memory_space_constraint(array, pltpu.HBM)


def pieces_of(width, sub=SUB):
    return [slice(j * sub, (j + 1) * sub) for j in range(width // sub)]


def times(width):
    return lax.broadcasted_iota(jnp.int32, (BLOCK, width), 0).astype(F32)


def squares_body(stream, squares):
    acc = jnp.zeros((stream.shape[0], 128), F32)
    for at in pieces_of(stream.shape[1], 128):
        x = stream[:, at].astype(F32)
        acc = acc + x * x
    squares[...] = jnp.sum(acc.T, axis=0, keepdims=True)


def gate_body(stream, inner, gain, v, *sent):
    start = 0
    for block in sent:
        for to in pieces_of(block.shape[1], 128):
            at = slice(start + to.start, start + to.stop)
            value = inner[:, at].astype(F32) * stream[:, at].astype(F32) * gain[:, at]
            v[:, at] = value.astype(BF16)
            block[:, to] = value.astype(BF16)
        start += block.shape[1]


def label_body(squares, beside, sent, total, out):
    value = squares[...] + beside[...]
    total[...] = value
    first = lax.broadcasted_iota(jnp.int32, (16, 128), 0) == 0
    for k in range(3):
        col = slice(k * 128, (k + 1) * 128)
        term = value.astype(BF16).astype(F32)
        value = value - term
        out[:, col] = jnp.where(first, term, sent[:, col].astype(F32)).astype(BF16)


def label(squares, beside, sent):
    rows, width = sent.shape
    part = pl.BlockSpec((16, 3 * 128), lambda i: (0, 0))
    row = pl.BlockSpec((1, rows), lambda i: (0, 0))
    return pl.pallas_call(
        label_body,
        grid=(1,),
        in_specs=[row, row, part],
        out_specs=[row, part],
        out_shape=[jax.ShapeDtypeStruct((1, rows), F32), jax.ShapeDtypeStruct((rows, width), BF16)],
        input_output_aliases={2: 1},
        compiler_params=pltpu.CompilerParams(vmem_limit_bytes=VMEM),
        name="label",
    )(squares, beside, sent)


def tables_body(forward, taps, inner, short_outer, decay, spectrum, gate):
    f_hi, f_lo = split(forward[:, :BLOCK])
    for at in pieces_of(taps.shape[1]):
        d = decay[:, at]
        spectrum[:, at] = dot(f_hi, taps[:, at]) + dot(f_lo, taps[:, at])
        time = times(SUB)
        gate[:, at] = inner[:, at].astype(F32) * short_outer[:, at].astype(F32) * jnp.exp(d * time)


def conv_first(
    before, here, squares, forward, back, lower, spectrum, gate, decay, far, state, matrix, summed, sems
):
    carried = before[:16, : 3 * 128].astype(F32)
    earlier = (carried[:1, :128] + carried[:1, 128:256]) + carried[:1, 256:]
    sums = jnp.concatenate([earlier, squares[...]], axis=1)
    column = lax.broadcasted_iota(jnp.int32, (1, 2 * BLOCK), 1)
    factor = jnp.where(column == 0, 0.0, 1.0 / jnp.sqrt(sums / D + 0.5))
    matrix[...] = (forward[...] * factor).astype(BF16)
    conv_body(0, before, here, matrix, back, lower, spectrum, gate, decay, far, state, summed, sems)


def conv_last(
    start, before, here, matrix, back, lower, spectrum, gate, decay, earlier, whole, far, copied, rows, summed, sems
):
    conv_body(start, before, here, matrix, back, lower, spectrum, gate, decay, far, rows, summed, sems)
    state = jnp.concatenate([earlier[...], rows[...]], axis=0).astype(BF16)
    for k in range(copied.shape[0]):
        copied[k] = state


def conv_body(
    start, before, here, matrix, back, lower, spectrum, gate, decay, far, state, summed, sems
):
    b = back[...].astype(BF16)
    leaving = []
    for j, to in enumerate(pieces_of(before.shape[1])):
        at = slice(start + to.start, start + to.stop)
        x = dot(matrix[...], jnp.concatenate([before[:, to], here[:, at]], axis=0))
        h = spectrum[:, at]
        x_re, x_im = x[:BLOCK], x[BLOCK:]
        h_re, h_im = h[:BLOCK], h[BLOCK:]
        y_re = (x_re * h_re - x_im * h_im).astype(BF16)
        y_im = (x_re * h_im + x_im * h_re).astype(BF16)
        conv = dot(b, jnp.concatenate([y_re, y_im], axis=0))
        z = (gate[:, at] * conv).astype(BF16)
        summed[:, to] = z
        leaving.append(
            pltpu.make_async_copy(
                summed.at[:, pl.ds(to.start, SUB)], far.at[:, pl.ds(at.start, SUB)], sems.at[j]
            )
        )
        leaving[-1].start()
        result = dot(lower[...], z)
        last = result[BLOCK - 1 :] * jnp.exp(decay[:, at] * (1.0 - BLOCK))
        for k in range(SUB // 128):
            row = j * (SUB // 128) + k
            state[row : row + 1, :] = last[:, k * 128 : (k + 1) * 128]
    for copy in leaving:
        copy.wait()


def weighted(pieces, place, rate, some=slice(None)):
    out = jnp.zeros(rate.shape, F32)
    for k in range(pieces.shape[0]):
        gap = place - 1 - k
        weight = jnp.exp(-rate * jnp.maximum(gap, 0).astype(F32))
        out = out + jnp.where(gap >= 0, weight * pieces[k, some].astype(F32), 0.0)
    return out


def near_body(place, pieces, rate, inside, copied):
    size, r = pieces.shape[0], rate[...]
    inside[...] = weighted(pieces, place[0], r)
    group = weighted(pieces, jnp.int32(size), r).astype(BF16)
    for k in range(copied.shape[0]):
        copied[k] = group


def early_body(summed_far, lower, outer_far, decay, scale, weights, sent, summed, long_outer, *sems):
    share = summed.shape[1]
    summed_in = fetches(summed_far, summed, sems[0], 0, PIECE)
    outer_in = fetches(outer_far, long_outer, sems[1], 0, PIECE)
    time = times(PIECE)
    for k, at in enumerate(pieces_of(share, PIECE)):
        d = decay[:, at]
        factor = jnp.exp(-d * time) * scale[:, at]
        summed_in[k].wait()
        base = dot(lower[...], summed[:, at])
        outer_in[k].wait()
        outer = long_outer[:, at].astype(F32) * factor
        value = (outer * base).astype(BF16)
        slope = (outer * jnp.exp(-d)).astype(BF16)
        for j, to in enumerate(pieces_of(PIECE, HEAD_DIM)):
            head = at.start // HEAD_DIM + j
            both = dot(weights[head], jnp.concatenate([value[:, to], slope[:, to]], axis=1))
            low = head * HEAD_DIM
            high = share + low
            sent[:, low : low + HEAD_DIM] = both[:, :HEAD_DIM].astype(BF16)
            sent[:, high : high + HEAD_DIM] = both[:, HEAD_DIM:].astype(BF16)


def finish_body(
    start,
    near_size,
    place,
    others,
    inside,
    rate,
    summed_far,
    lower,
    outer_far,
    decay,
    scale,
    weights,
    mixed,
    *rest,
):
    summed, long_outer, summed_sems, outer_sems = rest[-4:]
    summed_in = fetches(summed_far, summed, summed_sems, start, PIECE)
    outer_in = fetches(outer_far, long_outer, outer_sems, start, PIECE)
    near, far = place[0], place[1]
    r = rate[...]
    carry = inside[...] + jnp.exp(-r * near.astype(F32)) * weighted(others, far, r * near_size)
    time = times(PIECE)
    for k, to in enumerate(pieces_of(mixed.shape[1], PIECE)):
        at = slice(start + to.start, start + to.stop)
        d = decay[:, at]
        heads = range(at.start // HEAD_DIM, at.stop // HEAD_DIM)
        entering = jnp.concatenate([carry[j : j + 1] for j in heads], axis=1) * jnp.exp(-d)
        factor = jnp.exp(-d * time) * scale[:, at]
        summed_in[k].wait()
        base = dot(lower[...], summed[:, to]) + entering
        outer_in[k].wait()
        mixed[:, to] = (long_outer[:, to].astype(F32) * factor * base).astype(BF16)
    if start == 0:
        return
    ahead = rest[0]
    for j, to in enumerate(pieces_of(mixed.shape[1], HEAD_DIM)):
        head = start // HEAD_DIM + j
        ahead[:BLOCK, to] = dot(weights[head], mixed[:, to]).astype(BF16)
    if ahead.shape[0] > BLOCK:
        row = lax.broadcasted_iota(jnp.int32, (16, HEAD_DIM), 0)
        for j, to in enumerate(pieces_of(EARLY, HEAD_DIM)):
            left = carry[j : j + 1]
            kept = jnp.zeros((16, HEAD_DIM), F32)
            for k in range(3):
                term = left.astype(BF16).astype(F32)
                left = left - term
                kept = jnp.where(row == k, term, kept)
            ahead[BLOCK:, to] = kept.astype(BF16)


def score(query, key):
    return lax.dot_general(
        query, key, (((1,), (1,)), ((), ())), preferred_element_type=F32
    ) * HEAD_DIM ** (-0.5)


def soft(scores):
    top = jnp.max(scores, axis=1, keepdims=True)
    e = jnp.exp(scores - top)
    return e, top, jnp.sum(e, axis=1, keepdims=True)


def fetches(source, target, sems, first, width):
    copies = []
    for k in range(target.shape[1] // width):
        to = pl.ds(k * width, width)
        at = pl.ds(first + k * width, width)
        copies.append(pltpu.make_async_copy(source.at[:, at], target.at[:, to], sems.at[k]))
    for copy in copies:
        copy.start()
    return copies


def own_body(query_far, key_far, weights, stats, query, key, query_sems, key_sems):
    width = 2 * PIECE
    arriving = [
        pair
        for pair in zip(
            fetches(query_far, query, query_sems, 0, width),
            fetches(key_far, key, key_sems, 0, width),
        )
    ]
    row = lax.broadcasted_iota(jnp.int32, (BLOCK, BLOCK), 0)
    lane = lax.broadcasted_iota(jnp.int32, (BLOCK, BLOCK), 1)
    tops = jnp.zeros((BLOCK, BLOCK), F32)
    sizes = jnp.zeros((BLOCK, BLOCK), F32)
    for j in range(weights.shape[0]):
        at = slice(j * HEAD_DIM, (j + 1) * HEAD_DIM)
        if at.start % width == 0:
            for copy in arriving[at.start // width]:
                copy.wait()
        e, top, size = soft(jnp.where(lane <= row, score(query[:, at], key[:, at]), -1e30))
        weights[j] = e.astype(BF16)
        tops = jnp.where(lane == j, top, tops)
        sizes = jnp.where(lane == j + BLOCK // 2, size, sizes)
    stats[...] = jnp.where(lane < BLOCK // 2, tops, sizes)


def ahead_body(query, key_far, weights, stats, key, sems):
    width = 2 * PIECE
    arriving = fetches(key_far, key, sems, 0, width)
    lane = lax.broadcasted_iota(jnp.int32, (BLOCK, BLOCK), 1)
    tops = jnp.zeros((BLOCK, BLOCK), F32)
    sizes = jnp.zeros((BLOCK, BLOCK), F32)
    for j in range(weights.shape[0]):
        at = slice(j * HEAD_DIM, (j + 1) * HEAD_DIM)
        if at.start % width == 0:
            arriving[at.start // width].wait()
        e, top, size = soft(score(query[:, at], key[:, at]))
        weights[j] = (e * (1.0 / size)).astype(BF16)
        tops = jnp.where(lane == j, top, tops)
        sizes = jnp.where(lane == j + BLOCK // 2, size, sizes)
    stats[...] = jnp.where(lane < BLOCK // 2, tops, sizes)


def here_body(weights, first, middle, last, stats_here, stats_before, early, base, slope, share):
    top, size = stats_here[...], pltpu.roll(stats_here[...], BLOCK // 2, 1)
    size_b = pltpu.roll(stats_before[...], BLOCK // 2, 1)
    top_b = jnp.where(size_b > 0.0, stats_before[...], -1e30)
    highest = jnp.maximum(top, top_b)
    scale = jnp.exp(top - highest)
    scale_b = size_b * jnp.exp(top_b - highest)
    whole = 1.0 / (size * scale + scale_b)
    own, other = scale * whole, scale_b * whole
    share[...] = other
    start = 0
    for block in (first, middle, last):
        for to in pieces_of(block.shape[1], HEAD_DIM):
            at = slice(start + to.start, start + to.stop)
            j = at.start // HEAD_DIM
            part = dot(weights[j], block[:, to]) * own[:, j : j + 1]
            if start == 0:
                column = other[:, j : j + 1]
                part = part + column * early[:, to].astype(F32)
                up = slice(EARLY + to.start, EARLY + to.stop)
                slope[:, to] = column * early[:, up].astype(F32)
            base[:, at] = part
        start += block.shape[1]


def join_body(base, slope, share, before, last, attended, out, sems):
    leaving = []
    for k, at in enumerate(pieces_of(base.shape[1], PIECE)):
        for to in pieces_of(PIECE, HEAD_DIM):
            to = slice(at.start + to.start, at.start + to.stop)
            j = to.start // HEAD_DIM
            if to.start < EARLY:
                terms = before[BLOCK:, to].astype(F32)
                state = (terms[:1] + terms[1:2]) + terms[2:3]
                more = slope[:, to] * state
            elif to.start < MIDDLE:
                of = slice(to.start - EARLY, to.stop - EARLY)
                more = share[:, j : j + 1] * before[:BLOCK, of].astype(F32)
            else:
                of = slice(to.start - MIDDLE, to.stop - MIDDLE)
                more = share[:, j : j + 1] * last[:, of].astype(F32)
            out[:, to] = (base[:, to] + more).astype(BF16)
        at = pl.ds(at.start, PIECE)
        leaving.append(pltpu.make_async_copy(out.at[:, at], attended.at[:, at], sems.at[k]))
        leaving[-1].start()
    for copy in leaving:
        copy.wait()


def copy_body(block, *rest):
    rest[-1][...] = block[...]


def into(body, index, block, whole, width):
    rows, share = block.shape
    specs = [pl.BlockSpec((rows, share), lambda i: (0, 0))]
    operands, aliases = (block,), {}
    if whole is not None:
        specs.append(pl.BlockSpec(memory_space=pl.ANY))
        operands, aliases = (block, whole), {1: 0}
    return pl.pallas_call(
        body,
        grid=(1,),
        in_specs=specs,
        out_specs=pl.BlockSpec((rows, share), lambda i: (0, index)),
        out_shape=jax.ShapeDtypeStruct((rows, width), BF16),
        input_output_aliases=aliases,
        compiler_params=pltpu.CompilerParams(vmem_limit_bytes=VMEM),
    )(*operands)


def on_device(
    stream,
    norm_gain,
    short_outer,
    short_inner,
    short_filter,
    long_outer,
    long_inner,
    long_decay,
    query_heads,
    key_heads,
):
    rows, width = stream.shape
    heads, lanes = width // HEAD_DIM, width // 128
    decay = long_decay[None]
    scale = jnp.sqrt(-jnp.expm1(-2.0 * decay))
    rate = long_decay.reshape(lanes, 128) * rows
    near, far = lax.axis_index(NEAR), lax.axis_index(FAR)
    near_size, far_size = lax.axis_size(NEAR), lax.axis_size(FAR)
    forward, back = jnp.asarray(FORWARD), jnp.asarray(BACK)
    lower = jnp.asarray(np.tril(np.ones((rows, rows), np.float32)), BF16)
    square = ((rows, rows), F32)
    wide, wide_float = ((rows, width), BF16), ((rows, width), F32)

    (squares,) = call(squares_body, [((1, rows), F32)], operands=1)(stream)
    beside = swapped(squares)
    v, *sent = call(gate_body, [wide] + [((rows, share), BF16) for share in TAIL], operands=3)(
        stream, short_inner, norm_gain[None]
    )
    total, sent[0] = label(squares, beside, sent[0])
    v_before = []
    for part in range(len(TAIL)):
        v_before.append(shifted(sent[part], SEQ, 1))
    queries, total = lax.optimization_barrier((query_heads, total))
    query_next = shifted(queries, SEQ, -1)
    spectrum, gate = call(
        tables_body, [((2 * rows, width), F32), wide_float], operands=5
    )(forward, short_filter, long_inner, short_outer, decay)

    def leaving(share):
        return [pltpu.VMEM((rows, share), BF16), pltpu.SemaphoreType.DMA((share // SUB,))]

    summed, state, matrix = call(
        conv_first,
        [wide, ((TAIL[0] // 128, 128), F32), ((2 * rows, 2 * rows), BF16)],
        leaving(TAIL[0]),
        operands=9,
        kept=(0,),
    )(v_before[0], v, total, forward, back, lower, spectrum, gate, decay)
    summed, state = call(
        functools.partial(conv_last, TAIL[0]),
        [wide, ((near_size, lanes, 128), BF16)],
        [pltpu.VMEM((TAIL[1] // 128, 128), F32), *leaving(TAIL[1])],
        operands=10,
        outside=(9,),
        kept=(0,),
        aliases={9: 0},
    )(v_before[1], v, matrix, back, lower, spectrum, gate, decay, state, summed)
    pieces = lax.all_to_all(state, NEAR, 0, 0, tiled=True)
    weights_next, stats_next = call(
        ahead_body,
        [((heads, rows, rows), BF16), square],
        [pltpu.VMEM((rows, width), BF16), pltpu.SemaphoreType.DMA((width // PIECE // 2,))],
        operands=2,
        outside=(1,),
    )(query_next, in_hbm(key_heads))
    pieces, stats_next = lax.optimization_barrier((pieces, stats_next))
    inside, group = call(
        near_body, [((lanes, 128), F32), ((far_size, lanes, 128), BF16)], scalars=1, operands=2
    )(near[None], pieces, rate)
    others = lax.all_to_all(group, FAR, 0, 0, tiled=True)

    def fetching(share):
        space = [pltpu.VMEM((rows, share), BF16)] * 2
        return space + [pltpu.SemaphoreType.DMA((share // PIECE,))] * 2

    summed, inside = lax.optimization_barrier((summed, inside))
    (early,) = call(
        early_body, [((rows, 2 * EARLY), BF16)], fetching(EARLY), operands=6, outside=(0, 2)
    )(in_hbm(summed), lower, in_hbm(long_outer), decay, scale, weights_next)
    early = shifted(early, SEQ, 1)
    stats_before = shifted(stats_next, SEQ, 1)

    def finish(start, stop, extra):
        return call(
            functools.partial(finish_body, start, float(near_size)),
            [((rows, stop - start), BF16), *extra],
            fetching(stop - start),
            scalars=1,
            operands=9,
            outside=(4, 6),
        )(
            jnp.stack([near, far]),
            others,
            inside,
            rate,
            in_hbm(summed),
            lower,
            in_hbm(long_outer),
            decay,
            scale,
            weights_next,
        )

    middle, ready = finish(EARLY, MIDDLE, [((rows + 16, MIDDLE - EARLY), BF16)])
    arrived = shifted(ready, SEQ, 1)
    others, middle = lax.optimization_barrier((others, middle))
    last, ready = finish(MIDDLE, width, [((rows, width - MIDDLE), BF16)])
    arrived_last = shifted(ready, SEQ, 1)
    others, last = lax.optimization_barrier((others, last))
    (first,) = finish(0, EARLY, [])
    values = into(copy_body, 0, first, None, width)
    values = into(copy_body, EARLY // (MIDDLE - EARLY), middle, values, width)
    values = into(copy_body, MIDDLE // (width - MIDDLE), last, values, width)
    query_own, key_own, last = lax.optimization_barrier((query_heads, key_heads, last))
    weights_here, stats_here = call(
        own_body,
        [((heads, rows, rows), BF16), square],
        [pltpu.VMEM((rows, width), BF16)] * 2
        + [pltpu.SemaphoreType.DMA((width // PIECE // 2,))] * 2,
        operands=2,
        outside=(0, 1),
    )(in_hbm(query_own), in_hbm(key_own))
    base, slope, share = call(
        here_body, [wide_float, ((rows, EARLY), F32), square], operands=7
    )(weights_here, first, middle, last, stats_here, stats_before, early)
    (attended,) = call(
        join_body,
        [wide],
        [pltpu.VMEM((rows, width), BF16), pltpu.SemaphoreType.DMA((width // PIECE,))],
        operands=5,
        kept=(0,),
    )(base, slope, share, arrived, arrived_last)
    return (values, attended)


def solution(mesh):
    finer = Mesh(
        mesh.devices.reshape(8, 2, 4, 2, mesh.shape["mp"]),
        ("seq_0", "seq_1", "seq_2", "seq_3", "mp"),
    )
    placed = (
        P(SEQ, "mp"),
        P("mp"),
        P(SEQ, "mp"),
        P(SEQ, "mp"),
        P(None, "mp"),
        P(SEQ, "mp"),
        P(SEQ, "mp"),
        P("mp"),
        P(SEQ, "mp"),
        P(SEQ, "mp"),
    )
    return jax.shard_map(
        on_device,
        mesh=finer,
        in_specs=placed,
        out_specs=(P(SEQ, "mp"), P(SEQ, "mp")),
        check_vma=False,
    )
```

```python
import functools

import jax
import jax.numpy as jnp
import numpy as np
from jax import lax
from jax.experimental import pallas as pl
from jax.experimental.pallas import tpu as pltpu
from jax.sharding import Mesh
from jax.sharding import PartitionSpec as P

D = 8192
HEAD_DIM = 128
BLOCK = 128
SEQ = ("seq_0", "seq_1", "seq_2", "seq_3")
NEAR = ("seq_2", "seq_3")
FAR = ("seq_0", "seq_1")
F32 = jnp.float32
BF16 = jnp.bfloat16
SUB = 256
PIECE = 512
ROWS = 16
TAIL = (2560, 1536)
EARLY = 1024
MIDDLE = 2560
VMEM = 8 * 2**20


def dft_matrices():
    n = 2 * BLOCK
    k = np.arange(BLOCK, dtype=np.float64)[:, None]
    t = np.arange(n, dtype=np.float64)[None, :]
    angle = np.pi * (2 * k + 1) * t / n
    forward = np.concatenate([np.cos(angle), -np.sin(angle)], axis=0)
    back = np.concatenate([np.cos(angle), -np.sin(angle)], axis=0).T[BLOCK:] * (2.0 / n)
    return forward.astype(np.float32), back.astype(np.float32)


FORWARD, BACK = dft_matrices()


def split(value):
    high = value.astype(BF16)
    return high, (value - high.astype(F32)).astype(BF16)


def dot(a, b):
    return jnp.dot(a, b, preferred_element_type=F32)


def shifted(block, axis, distance):
    size = lax.axis_size(axis)
    return lax.ppermute(block, axis, [(i, i + distance) for i in range(size) if 0 <= i + distance < size])


def swapped(block):
    sides = lax.axis_size("mp")
    return lax.ppermute(block, "mp", [(m, sides - 1 - m) for m in range(sides)])


def call(body, outs, scratch=(), scalars=0, operands=0, flops=10**8, outside=(), kept=()):
    specs = [pl.BlockSpec(memory_space=pltpu.SMEM)] * scalars
    specs += [pl.BlockSpec(memory_space=pltpu.VMEM)] * operands
    for k in outside:
        specs[k] = pl.BlockSpec(memory_space=pltpu.HBM)
    return pl.pallas_call(
        body,
        in_specs=specs,
        out_specs=[
            pl.BlockSpec(memory_space=pltpu.HBM if k in kept else pltpu.VMEM)
            for k in range(len(outs))
        ],
        out_shape=[
            pltpu.HBM(shape, kind) if k in kept else jax.ShapeDtypeStruct(shape, kind)
            for k, (shape, kind) in enumerate(outs)
        ],
        scratch_shapes=list(scratch),
        compiler_params=pltpu.CompilerParams(vmem_limit_bytes=VMEM),
        cost_estimate=pl.CostEstimate(flops=flops, transcendentals=0, bytes_accessed=10**6),
    )


def in_hbm(array):
    return pltpu.with_memory_space_constraint(array, pltpu.HBM)


def pieces_of(width, sub=SUB):
    return [slice(j * sub, (j + 1) * sub) for j in range(width // sub)]


def times(width):
    return lax.broadcasted_iota(jnp.int32, (BLOCK, width), 0).astype(F32)


def squares_body(stream_far, squares, stream, sems):
    arriving = rows_in(stream_far, stream, sems)
    parts = []
    for k, copy in enumerate(arriving):
        copy.wait()
        part = jnp.zeros((ROWS, 128), F32)
        for at in pieces_of(stream.shape[1], 128):
            x = stream[k * ROWS : (k + 1) * ROWS, at].astype(F32)
            part = part + x * x
        parts.append(part)
    squares[...] = jnp.sum(jnp.concatenate(parts, axis=0).T, axis=0, keepdims=True)


def rows_in(source, target, sems):
    copies = []
    for k in range(target.shape[0] // ROWS):
        at = pl.ds(k * ROWS, ROWS)
        copies.append(pltpu.make_async_copy(source.at[at], target.at[at], sems.at[k]))
        copies[-1].start()
    return copies


def gate_body(stream, inner_far, gain_far, v, *rest):
    sent, (inner, gain, sems, sem) = rest[:-4], rest[-4:]
    copy = pltpu.make_async_copy(gain_far, gain, sem)
    copy.start()
    arriving = rows_in(inner_far, inner, sems)
    copy.wait()
    for k in range(len(arriving)):
        arriving[k].wait()
        row = slice(k * ROWS, (k + 1) * ROWS)
        start = 0
        for block in sent:
            for to in pieces_of(block.shape[1], 128):
                at = slice(start + to.start, start + to.stop)
                value = inner[row, at].astype(F32) * stream[row, at].astype(F32) * gain[:, at]
                v[row, at] = value.astype(BF16)
                block[row, to] = value.astype(BF16)
            start += block.shape[1]


def label_body(squares, beside, sent, total, out):
    value = squares[...] + beside[...]
    total[...] = value
    first = lax.broadcasted_iota(jnp.int32, (16, 128), 0) == 0
    for k in range(3):
        col = slice(k * 128, (k + 1) * 128)
        term = value.astype(BF16).astype(F32)
        value = value - term
        out[:, col] = jnp.where(first, term, sent[:, col].astype(F32)).astype(BF16)


def label(squares, beside, sent):
    rows, width = sent.shape
    part = pl.BlockSpec((16, 3 * 128), lambda i: (0, 0))
    row = pl.BlockSpec((1, rows), lambda i: (0, 0))
    return pl.pallas_call(
        label_body,
        grid=(1,),
        in_specs=[row, row, part],
        out_specs=[row, part],
        out_shape=[jax.ShapeDtypeStruct((1, rows), F32), jax.ShapeDtypeStruct((rows, width), BF16)],
        input_output_aliases={2: 1},
        compiler_params=pltpu.CompilerParams(vmem_limit_bytes=VMEM),
        name="label",
    )(squares, beside, sent)


def tables_body(forward, taps, inner, short_outer, decay, spectrum, gate):
    f_hi, f_lo = split(forward[:, :BLOCK])
    for at in pieces_of(taps.shape[1]):
        d = decay[:, at]
        spectrum[:, at] = dot(f_hi, taps[:, at]) + dot(f_lo, taps[:, at])
        time = times(SUB)
        gate[:, at] = inner[:, at].astype(F32) * short_outer[:, at].astype(F32) * jnp.exp(d * time)


def conv_first(
    before, here, squares, forward, back, lower, spectrum, gate, decay, far, state, matrix, summed, sems
):
    carried = before[:16, : 3 * 128].astype(F32)
    earlier = (carried[:1, :128] + carried[:1, 128:256]) + carried[:1, 256:]
    sums = jnp.concatenate([earlier, squares[...]], axis=1)
    column = lax.broadcasted_iota(jnp.int32, (1, 2 * BLOCK), 1)
    factor = jnp.where(column == 0, 0.0, 1.0 / jnp.sqrt(sums / D + 0.5))
    matrix[...] = (forward[...] * factor).astype(BF16)
    leaving = []

    def done(j, to):
        at = pl.ds(to.start, SUB)
        leaving.append(pltpu.make_async_copy(summed.at[:, at], far.at[:, at], sems.at[j]))
        leaving[-1].start()

    conv_body(0, before, here, matrix, back, lower, spectrum, gate, decay, summed, state, done)
    for copy in leaving:
        copy.wait()


def conv_last(
    start, before, here, matrix, back, lower, spectrum, gate, decay, earlier, summed, copied, state
):
    state[: start // 128, :] = earlier[...]
    conv_body(start, before, here, matrix, back, lower, spectrum, gate, decay, summed, state)
    rows = state[...].astype(BF16)
    for k in range(copied.shape[0]):
        copied[k] = rows


def conv_body(
    start, before, here, matrix, back, lower, spectrum, gate, decay, summed, state, done=None
):
    b = back[...].astype(BF16)
    for j, to in enumerate(pieces_of(before.shape[1])):
        at = slice(start + to.start, start + to.stop)
        x = dot(matrix[...], jnp.concatenate([before[:, to], here[:, at]], axis=0))
        h = spectrum[:, at]
        x_re, x_im = x[:BLOCK], x[BLOCK:]
        h_re, h_im = h[:BLOCK], h[BLOCK:]
        y_re = (x_re * h_re - x_im * h_im).astype(BF16)
        y_im = (x_re * h_im + x_im * h_re).astype(BF16)
        conv = dot(b, jnp.concatenate([y_re, y_im], axis=0))
        z = (gate[:, at] * conv).astype(BF16)
        summed[:, to] = z
        if done is not None:
            done(j, to)
        result = dot(lower[...], z)
        last = result[BLOCK - 1 :] * jnp.exp(decay[:, at] * (1.0 - BLOCK))
        for k in range(SUB // 128):
            row = at.start // 128 + k
            state[row : row + 1, :] = last[:, k * 128 : (k + 1) * 128]


def weighted(pieces, place, rate, some=slice(None)):
    out = jnp.zeros(rate.shape, F32)
    for k in range(pieces.shape[0]):
        gap = place - 1 - k
        weight = jnp.exp(-rate * jnp.maximum(gap, 0).astype(F32))
        out = out + jnp.where(gap >= 0, weight * pieces[k, some].astype(F32), 0.0)
    return out


def near_body(place, pieces, rate, inside, copied):
    size, r = pieces.shape[0], rate[...]
    inside[...] = weighted(pieces, place[0], r)
    group = weighted(pieces, jnp.int32(size), r).astype(BF16)
    for k in range(copied.shape[0]):
        copied[k] = group


def early_body(
    summed_far,
    lower,
    outer_far,
    decay,
    scale,
    weights,
    stats,
    sent,
    summed_middle,
    outer_middle,
    summed,
    long_outer,
    *sems,
):
    share = summed.shape[1]
    summed_in = fetches(summed_far, summed, sems[0], 0, PIECE)
    outer_in = fetches(outer_far, long_outer, sems[1], 0, PIECE)
    left = stats[...]
    for k in range(3):
        term = left.astype(BF16)
        left = left - term.astype(F32)
        low = 2 * share + k * BLOCK
        sent[:, low : low + BLOCK] = term
    later = fetches(summed_far, summed_middle, sems[2], EARLY, PIECE)
    later += fetches(outer_far, outer_middle, sems[3], EARLY, PIECE)
    time = times(PIECE)
    for k, at in enumerate(pieces_of(share, PIECE)):
        d = decay[:, at]
        factor = jnp.exp(-d * time) * scale[:, at]
        summed_in[k].wait()
        base = dot(lower[...], summed[:, at])
        outer_in[k].wait()
        outer = long_outer[:, at].astype(F32) * factor
        value = (outer * base).astype(BF16)
        slope = (outer * jnp.exp(-d)).astype(BF16)
        for j, to in enumerate(pieces_of(PIECE, HEAD_DIM)):
            head = at.start // HEAD_DIM + j
            both = dot(weights[head], jnp.concatenate([value[:, to], slope[:, to]], axis=1))
            low = head * HEAD_DIM
            high = share + low
            sent[:, low : low + HEAD_DIM] = both[:, :HEAD_DIM].astype(BF16)
            sent[:, high : high + HEAD_DIM] = both[:, HEAD_DIM:].astype(BF16)
    for copy in later:
        copy.wait()


def finish(start, near_size, place, others, inside, rate, lower, decay, scale, mixed, read):
    near, far = place[0], place[1]
    r = rate[...]
    carry = inside[...] + jnp.exp(-r * near.astype(F32)) * weighted(others, far, r * near_size)
    time = times(PIECE)
    for k, to in enumerate(pieces_of(mixed.shape[1], PIECE)):
        at = slice(start + to.start, start + to.stop)
        d = decay[:, at]
        heads = range(at.start // HEAD_DIM, at.stop // HEAD_DIM)
        entering = jnp.concatenate([carry[j : j + 1] for j in heads], axis=1) * jnp.exp(-d)
        factor = jnp.exp(-d * time) * scale[:, at]
        summed, outer = read(k, to)
        base = dot(lower[...], summed) + entering
        mixed[:, to] = (outer.astype(F32) * factor * base).astype(BF16)
    return carry


def finish_first(
    near_size, place, others, inside, rate, summed_far, lower, outer_far, decay, scale, mixed, *rest
):
    summed, outer, summed_sems, outer_sems = rest
    summed_in = fetches(summed_far, summed, summed_sems, 0, PIECE)
    outer_in = fetches(outer_far, outer, outer_sems, 0, PIECE)

    def read(k, to):
        summed_in[k].wait()
        outer_in[k].wait()
        return summed[:, to], outer[:, to]

    finish(0, near_size, place, others, inside, rate, lower, decay, scale, mixed, read)


def partial_attention(start, weights, mixed, ahead):
    for j, to in enumerate(pieces_of(mixed.shape[1], HEAD_DIM)):
        head = start // HEAD_DIM + j
        ahead[:BLOCK, to] = dot(weights[head], mixed[:, to]).astype(BF16)


def finish_middle(
    near_size,
    place,
    others,
    inside,
    rate,
    summed,
    lower,
    outer,
    decay,
    scale,
    weights,
    mixed,
    ahead,
):
    carry = finish(
        EARLY,
        near_size,
        place,
        others,
        inside,
        rate,
        lower,
        decay,
        scale,
        mixed,
        lambda k, to: (summed[:, to], outer[:, to]),
    )
    partial_attention(EARLY, weights, mixed, ahead)
    row = lax.broadcasted_iota(jnp.int32, (16, HEAD_DIM), 0)
    for j, to in enumerate(pieces_of(ahead.shape[1], HEAD_DIM)):
        kept = jnp.zeros((16, HEAD_DIM), F32)
        if to.start < EARLY:
            left = carry[j : j + 1]
            for k in range(3):
                term = left.astype(BF16).astype(F32)
                left = left - term
                kept = jnp.where(row == k, term, kept)
        ahead[BLOCK:, to] = kept.astype(BF16)


def finish_last(
    near_size,
    place,
    others,
    inside,
    rate,
    summed,
    lower,
    outer_far,
    decay,
    scale,
    weights,
    mixed,
    ahead,
    outer,
    sems,
):
    outer_in = fetches(outer_far, outer, sems, MIDDLE, PIECE)

    def read(k, to):
        outer_in[k].wait()
        return summed[:, to], outer[:, to]

    finish(MIDDLE, near_size, place, others, inside, rate, lower, decay, scale, mixed, read)
    partial_attention(MIDDLE, weights, mixed, ahead)


def store_body(first, middle, last, whole, sems):
    leaving, start = [], 0
    for k, block in enumerate((first, middle, last)):
        share = block.shape[1]
        leaving.append(pltpu.make_async_copy(block, whole.at[:, pl.ds(start, share)], sems.at[k]))
        leaving[-1].start()
        start += share
    for copy in leaving:
        copy.wait()


def score(query, key):
    return lax.dot_general(
        query, key, (((1,), (1,)), ((), ())), preferred_element_type=F32
    ) * HEAD_DIM ** (-0.5)


def soft(scores):
    top = jnp.max(scores, axis=1, keepdims=True)
    e = jnp.exp(scores - top)
    return e, top, jnp.sum(e, axis=1, keepdims=True)


def fetches(source, target, sems, first, width):
    copies = []
    for k in range(target.shape[1] // width):
        to = pl.ds(k * width, width)
        at = pl.ds(first + k * width, width)
        copies.append(pltpu.make_async_copy(source.at[:, at], target.at[:, to], sems.at[k]))
    for copy in copies:
        copy.start()
    return copies


def own_body(query_far, key_far, weights, stats, query, key, query_sems, key_sems):
    width = 2 * PIECE
    arriving = [
        pair
        for pair in zip(
            fetches(query_far, query, query_sems, 0, width),
            fetches(key_far, key, key_sems, 0, width),
        )
    ]
    row = lax.broadcasted_iota(jnp.int32, (BLOCK, BLOCK), 0)
    lane = lax.broadcasted_iota(jnp.int32, (BLOCK, BLOCK), 1)
    tops = jnp.zeros((BLOCK, BLOCK), F32)
    sizes = jnp.zeros((BLOCK, BLOCK), F32)
    for j in range(weights.shape[0]):
        at = slice(j * HEAD_DIM, (j + 1) * HEAD_DIM)
        if at.start % width == 0:
            for copy in arriving[at.start // width]:
                copy.wait()
        e, top, size = soft(jnp.where(lane <= row, score(query[:, at], key[:, at]), -1e30))
        weights[j] = e.astype(BF16)
        tops = jnp.where(lane == j, top, tops)
        sizes = jnp.where(lane == j + BLOCK // 2, size, sizes)
    stats[...] = jnp.where(lane < BLOCK // 2, tops, sizes)


def ahead_body(query, key_far, weights, stats, key, sems):
    width = 2 * PIECE
    arriving = fetches(key_far, key, sems, 0, width)
    lane = lax.broadcasted_iota(jnp.int32, (BLOCK, BLOCK), 1)
    tops = jnp.zeros((BLOCK, BLOCK), F32)
    sizes = jnp.zeros((BLOCK, BLOCK), F32)
    for j in range(weights.shape[0]):
        at = slice(j * HEAD_DIM, (j + 1) * HEAD_DIM)
        if at.start % width == 0:
            arriving[at.start // width].wait()
        e, top, size = soft(score(query[:, at], key[:, at]))
        weights[j] = (e * (1.0 / size)).astype(BF16)
        tops = jnp.where(lane == j, top, tops)
        sizes = jnp.where(lane == j + BLOCK // 2, size, sizes)
    stats[...] = jnp.where(lane < BLOCK // 2, tops, sizes)


def here_body(weights, first, middle, last, stats_here, early, base, slope, share):
    top, size = stats_here[...], pltpu.roll(stats_here[...], BLOCK // 2, 1)
    terms = early[:, 2 * EARLY :].astype(F32)
    stats_before = (terms[:, :BLOCK] + terms[:, BLOCK : 2 * BLOCK]) + terms[:, 2 * BLOCK :]
    size_b = pltpu.roll(stats_before, BLOCK // 2, 1)
    top_b = jnp.where(size_b > 0.0, stats_before, -1e30)
    highest = jnp.maximum(top, top_b)
    scale = jnp.exp(top - highest)
    scale_b = size_b * jnp.exp(top_b - highest)
    whole = 1.0 / (size * scale + scale_b)
    own, other = scale * whole, scale_b * whole
    share[...] = other
    start = 0
    for block in (first, middle, last):
        for to in pieces_of(block.shape[1], HEAD_DIM):
            at = slice(start + to.start, start + to.stop)
            j = at.start // HEAD_DIM
            part = dot(weights[j], block[:, to]) * own[:, j : j + 1]
            if start == 0:
                column = other[:, j : j + 1]
                part = part + column * early[:, to].astype(F32)
                up = slice(EARLY + to.start, EARLY + to.stop)
                slope[:, to] = column * early[:, up].astype(F32)
            base[:, at] = part
        start += block.shape[1]


def join_body(base, slope, share, before, last, attended, out, sems):
    leaving = []
    for k, at in enumerate(pieces_of(base.shape[1], PIECE)):
        for to in pieces_of(PIECE, HEAD_DIM):
            to = slice(at.start + to.start, at.start + to.stop)
            j = to.start // HEAD_DIM
            if to.start < EARLY:
                terms = before[BLOCK:, to].astype(F32)
                state = (terms[:1] + terms[1:2]) + terms[2:3]
                more = slope[:, to] * state
            elif to.start < MIDDLE:
                of = slice(to.start - EARLY, to.stop - EARLY)
                more = share[:, j : j + 1] * before[:BLOCK, of].astype(F32)
            else:
                of = slice(to.start - MIDDLE, to.stop - MIDDLE)
                more = share[:, j : j + 1] * last[:, of].astype(F32)
            out[:, to] = (base[:, to] + more).astype(BF16)
        at = pl.ds(at.start, PIECE)
        leaving.append(pltpu.make_async_copy(out.at[:, at], attended.at[:, at], sems.at[k]))
        leaving[-1].start()
    for copy in leaving:
        copy.wait()


def on_device(
    stream,
    norm_gain,
    short_outer,
    short_inner,
    short_filter,
    long_outer,
    long_inner,
    long_decay,
    query_heads,
    key_heads,
):
    rows, width = stream.shape
    heads, lanes = width // HEAD_DIM, width // 128
    decay = long_decay[None]
    scale = jnp.sqrt(-jnp.expm1(-2.0 * decay))
    rate = long_decay.reshape(lanes, 128) * rows
    near, far = lax.axis_index(NEAR), lax.axis_index(FAR)
    near_size, far_size = lax.axis_size(NEAR), lax.axis_size(FAR)
    forward, back = jnp.asarray(FORWARD), jnp.asarray(BACK)
    lower = jnp.asarray(np.tril(np.ones((rows, rows), np.float32)), BF16)
    square = ((rows, rows), F32)
    wide, wide_float = ((rows, width), BF16), ((rows, width), F32)

    row_sems = pltpu.SemaphoreType.DMA((rows // ROWS,))
    squares, stream = call(
        squares_body, [((1, rows), F32), wide], [row_sems], operands=1, outside=(0,)
    )(in_hbm(stream))
    beside = swapped(squares)
    v, *sent = call(
        gate_body,
        [wide] + [((rows, share), BF16) for share in TAIL],
        [
            pltpu.VMEM((rows, width), BF16),
            pltpu.VMEM((1, width), F32),
            row_sems,
            pltpu.SemaphoreType.DMA,
        ],
        operands=3,
        outside=(1, 2),
    )(stream, in_hbm(short_inner), in_hbm(norm_gain[None]))
    total, sent[0] = label(squares, beside, sent[0])
    v_before = []
    for part in range(len(TAIL)):
        v_before.append(shifted(sent[part], SEQ, 1))
    queries, total = lax.optimization_barrier((query_heads, total))
    query_next = shifted(queries, SEQ, -1)
    spectrum, gate = call(
        tables_body, [((2 * rows, width), F32), wide_float], operands=5
    )(forward, short_filter, long_inner, short_outer, decay)
    summed, state, matrix = call(
        conv_first,
        [((rows, TAIL[0]), BF16), ((TAIL[0] // 128, 128), F32), ((2 * rows, 2 * rows), BF16)],
        [pltpu.VMEM((rows, TAIL[0]), BF16), pltpu.SemaphoreType.DMA((TAIL[0] // SUB,))],
        operands=9,
        kept=(0,),
    )(v_before[0], v, total, forward, back, lower, spectrum, gate, decay)
    summed_last, state = call(
        functools.partial(conv_last, TAIL[0]),
        [((rows, TAIL[1]), BF16), ((near_size, lanes, 128), BF16)],
        [pltpu.VMEM((lanes, 128), F32)],
        operands=9,
    )(v_before[1], v, matrix, back, lower, spectrum, gate, decay, state)
    pieces = lax.all_to_all(state, NEAR, 0, 0, tiled=True)
    weights_next, stats_next = call(
        ahead_body,
        [((heads, rows, rows), BF16), square],
        [pltpu.VMEM((rows, width), BF16), pltpu.SemaphoreType.DMA((width // PIECE // 2,))],
        operands=2,
        outside=(1,),
    )(query_next, in_hbm(key_heads))
    pieces, stats_next = lax.optimization_barrier((pieces, stats_next))
    inside, group = call(
        near_body, [((lanes, 128), F32), ((far_size, lanes, 128), BF16)], scalars=1, operands=2
    )(near[None], pieces, rate)
    others = lax.all_to_all(group, FAR, 0, 0, tiled=True)

    def fetching(share):
        space = [pltpu.VMEM((rows, share), BF16)] * 2
        return space + [pltpu.SemaphoreType.DMA((share // PIECE,))] * 2

    share = MIDDLE - EARLY
    middle_wide, last_wide = ((rows, share), BF16), ((rows, width - MIDDLE), BF16)
    summed, inside = lax.optimization_barrier((summed, inside))
    summed, outer = in_hbm(summed), in_hbm(long_outer)
    early, summed_middle, outer_middle = call(
        early_body,
        [((rows, 2 * EARLY + 3 * rows), BF16), middle_wide, middle_wide],
        fetching(EARLY) + [pltpu.SemaphoreType.DMA((share // PIECE,))] * 2,
        operands=7,
        outside=(0, 2),
    )(summed, lower, outer, decay, scale, weights_next, stats_next)
    early = shifted(early, SEQ, 1)
    place, steps = jnp.stack([near, far]), float(near_size)
    middle, ready = call(
        functools.partial(finish_middle, steps),
        [middle_wide, ((rows + 16, share), BF16)],
        scalars=1,
        operands=9,
    )(
        place, others, inside, rate, summed_middle, lower, outer_middle, decay, scale, weights_next
    )
    arrived = shifted(ready, SEQ, 1)
    last, ready = call(
        functools.partial(finish_last, steps),
        [last_wide, last_wide],
        [
            pltpu.VMEM((rows, width - MIDDLE), BF16),
            pltpu.SemaphoreType.DMA(((width - MIDDLE) // PIECE,)),
        ],
        scalars=1,
        operands=9,
        outside=(6,),
    )(place, others, inside, rate, summed_last, lower, outer, decay, scale, weights_next)
    arrived_last = shifted(ready, SEQ, 1)
    others, last = lax.optimization_barrier((others, last))
    (first,) = call(
        functools.partial(finish_first, steps),
        [((rows, EARLY), BF16)],
        fetching(EARLY),
        scalars=1,
        operands=8,
        outside=(4, 6),
    )(place, others, inside, rate, summed, lower, outer, decay, scale)
    (values,) = call(
        store_body, [wide], [pltpu.SemaphoreType.DMA((3,))], operands=3, kept=(0,)
    )(first, middle, last)
    query_own, key_own, last = lax.optimization_barrier((query_heads, key_heads, last))
    weights_here, stats_here = call(
        own_body,
        [((heads, rows, rows), BF16), square],
        [pltpu.VMEM((rows, width), BF16)] * 2
        + [pltpu.SemaphoreType.DMA((width // PIECE // 2,))] * 2,
        operands=2,
        outside=(0, 1),
    )(in_hbm(query_own), in_hbm(key_own))
    base, slope, share = call(
        here_body, [wide_float, ((rows, EARLY), F32), square], operands=6
    )(weights_here, first, middle, last, stats_here, early)
    (attended,) = call(
        join_body,
        [wide],
        [pltpu.VMEM((rows, width), BF16), pltpu.SemaphoreType.DMA((width // PIECE,))],
        operands=5,
        kept=(0,),
    )(base, slope, share, arrived, arrived_last)
    return (values, attended)


def solution(mesh):
    finer = Mesh(
        mesh.devices.reshape(8, 2, 4, 2, mesh.shape["mp"]),
        ("seq_0", "seq_1", "seq_2", "seq_3", "mp"),
    )
    placed = (
        P(SEQ, "mp"),
        P("mp"),
        P(SEQ, "mp"),
        P(SEQ, "mp"),
        P(None, "mp"),
        P(SEQ, "mp"),
        P(SEQ, "mp"),
        P("mp"),
        P(SEQ, "mp"),
        P(SEQ, "mp"),
    )
    return jax.shard_map(
        on_device,
        mesh=finer,
        in_specs=placed,
        out_specs=(P(SEQ, "mp"), P(SEQ, "mp")),
        check_vma=False,
    )
```

```python
import functools

import jax
import jax.numpy as jnp
import numpy as np
from jax import lax
from jax.experimental import pallas as pl
from jax.experimental.pallas import tpu as pltpu
from jax.sharding import Mesh
from jax.sharding import PartitionSpec as P

D = 8192
HEAD_DIM = 128
BLOCK = 128
SEQ = ("seq_0", "seq_1", "seq_2", "seq_3")
NEAR = ("seq_2", "seq_3")
FAR = ("seq_0", "seq_1")
F32 = jnp.float32
BF16 = jnp.bfloat16
SUB = 256
PIECE = 512
ROWS = 16
TAIL = (2560, 1536)
EARLY = 1024
MIDDLE = 2560
GROUP = 8
VMEM = 8 * 2**20


def dft_matrices():
    n = 2 * BLOCK
    k = np.arange(BLOCK, dtype=np.float64)[:, None]
    t = np.arange(n, dtype=np.float64)[None, :]
    angle = np.pi * (2 * k + 1) * t / n
    forward = np.concatenate([np.cos(angle), -np.sin(angle)], axis=0)
    back = np.concatenate([np.cos(angle), -np.sin(angle)], axis=0).T[BLOCK:] * (2.0 / n)
    return forward.astype(np.float32), back.astype(np.float32)


FORWARD, BACK = dft_matrices()


def split(value):
    high = value.astype(BF16)
    return high, (value - high.astype(F32)).astype(BF16)


def dot(a, b):
    return jnp.dot(a, b, preferred_element_type=F32)


def shifted(block, axis, distance):
    size = lax.axis_size(axis)
    return lax.ppermute(block, axis, [(i, i + distance) for i in range(size) if 0 <= i + distance < size])


def swapped(block):
    sides = lax.axis_size("mp")
    return lax.ppermute(block, "mp", [(m, sides - 1 - m) for m in range(sides)])


def call(body, outs, scratch=(), scalars=0, operands=0, flops=10**8, outside=(), kept=(), aliases={}):
    specs = [pl.BlockSpec(memory_space=pltpu.SMEM)] * scalars
    specs += [pl.BlockSpec(memory_space=pltpu.VMEM)] * operands
    for k in outside:
        specs[k] = pl.BlockSpec(memory_space=pltpu.HBM)
    return pl.pallas_call(
        body,
        in_specs=specs,
        out_specs=[
            pl.BlockSpec(memory_space=pltpu.HBM if k in kept else pltpu.VMEM)
            for k in range(len(outs))
        ],
        out_shape=[
            pltpu.HBM(shape, kind) if k in kept else jax.ShapeDtypeStruct(shape, kind)
            for k, (shape, kind) in enumerate(outs)
        ],
        scratch_shapes=list(scratch),
        input_output_aliases=aliases,
        compiler_params=pltpu.CompilerParams(vmem_limit_bytes=VMEM),
        cost_estimate=pl.CostEstimate(flops=flops, transcendentals=0, bytes_accessed=10**6),
    )


def in_hbm(array):
    return pltpu.with_memory_space_constraint(array, pltpu.HBM)


def pieces_of(width, sub=SUB):
    return [slice(j * sub, (j + 1) * sub) for j in range(width // sub)]


def times(width):
    return lax.broadcasted_iota(jnp.int32, (BLOCK, width), 0).astype(F32)


def squares_body(stream_far, squares, stream, sems):
    arriving = rows_in(stream_far, stream, sems)
    parts = []
    for k, copy in enumerate(arriving):
        copy.wait()
        part = jnp.zeros((ROWS, 128), F32)
        for at in pieces_of(stream.shape[1], 128):
            x = stream[k * ROWS : (k + 1) * ROWS, at].astype(F32)
            part = part + x * x
        parts.append(part)
    squares[...] = jnp.sum(jnp.concatenate(parts, axis=0).T, axis=0, keepdims=True)


def rows_in(source, target, sems):
    copies = []
    for k in range(target.shape[0] // ROWS):
        at = pl.ds(k * ROWS, ROWS)
        copies.append(pltpu.make_async_copy(source.at[at], target.at[at], sems.at[k]))
        copies[-1].start()
    return copies


def gate_body(stream, inner_far, gain_far, v, *rest):
    sent, (inner, gain, sems, sem) = rest[:-4], rest[-4:]
    copy = pltpu.make_async_copy(gain_far, gain, sem)
    copy.start()
    arriving = rows_in(inner_far, inner, sems)
    copy.wait()
    for k in range(len(arriving)):
        arriving[k].wait()
        row = slice(k * ROWS, (k + 1) * ROWS)
        start = 0
        for block in sent:
            for to in pieces_of(block.shape[1], 128):
                at = slice(start + to.start, start + to.stop)
                value = inner[row, at].astype(F32) * stream[row, at].astype(F32) * gain[:, at]
                v[row, at] = value.astype(BF16)
                block[row, to] = value.astype(BF16)
            start += block.shape[1]


def label_body(squares, beside, sent, total, out):
    value = squares[...] + beside[...]
    total[...] = value
    first = lax.broadcasted_iota(jnp.int32, (16, 128), 0) == 0
    for k in range(3):
        col = slice(k * 128, (k + 1) * 128)
        term = value.astype(BF16).astype(F32)
        value = value - term
        out[:, col] = jnp.where(first, term, sent[:, col].astype(F32)).astype(BF16)


def label(squares, beside, sent):
    rows, width = sent.shape
    part = pl.BlockSpec((16, 3 * 128), lambda i: (0, 0))
    row = pl.BlockSpec((1, rows), lambda i: (0, 0))
    return pl.pallas_call(
        label_body,
        grid=(1,),
        in_specs=[row, row, part],
        out_specs=[row, part],
        out_shape=[jax.ShapeDtypeStruct((1, rows), F32), jax.ShapeDtypeStruct((rows, width), BF16)],
        input_output_aliases={2: 1},
        compiler_params=pltpu.CompilerParams(vmem_limit_bytes=VMEM),
        name="label",
    )(squares, beside, sent)


def tables_body(forward, taps, inner, short_outer, decay, spectrum, gate):
    f_hi, f_lo = split(forward[:, :BLOCK])
    for at in pieces_of(taps.shape[1]):
        d = decay[:, at]
        spectrum[:, at] = dot(f_hi, taps[:, at]) + dot(f_lo, taps[:, at])
        time = times(SUB)
        gate[:, at] = inner[:, at].astype(F32) * short_outer[:, at].astype(F32) * jnp.exp(d * time)


def conv_first(
    before, here, squares, forward, back, lower, spectrum, gate, decay, far, state, matrix, summed, sems
):
    carried = before[:16, : 3 * 128].astype(F32)
    earlier = (carried[:1, :128] + carried[:1, 128:256]) + carried[:1, 256:]
    sums = jnp.concatenate([earlier, squares[...]], axis=1)
    column = lax.broadcasted_iota(jnp.int32, (1, 2 * BLOCK), 1)
    factor = jnp.where(column == 0, 0.0, 1.0 / jnp.sqrt(sums / D + 0.5))
    matrix[...] = (forward[...] * factor).astype(BF16)
    leaving = []

    def done(j, to):
        at = pl.ds(to.start, SUB)
        leaving.append(pltpu.make_async_copy(summed.at[:, at], far.at[:, at], sems.at[j]))
        leaving[-1].start()

    conv_body(0, before, here, matrix, back, lower, spectrum, gate, decay, summed, state, done)
    for copy in leaving:
        copy.wait()


def conv_last(
    start, before, here, matrix, back, lower, spectrum, gate, decay, earlier, summed, copied, state
):
    state[: start // 128, :] = earlier[...]
    conv_body(start, before, here, matrix, back, lower, spectrum, gate, decay, summed, state)
    rows = state[...].astype(BF16)
    for k in range(copied.shape[0]):
        copied[k] = rows


def conv_body(
    start, before, here, matrix, back, lower, spectrum, gate, decay, summed, state, done=None
):
    b = back[...].astype(BF16)
    for j, to in enumerate(pieces_of(before.shape[1])):
        at = slice(start + to.start, start + to.stop)
        x = dot(matrix[...], jnp.concatenate([before[:, to], here[:, at]], axis=0))
        h = spectrum[:, at]
        x_re, x_im = x[:BLOCK], x[BLOCK:]
        h_re, h_im = h[:BLOCK], h[BLOCK:]
        y_re = (x_re * h_re - x_im * h_im).astype(BF16)
        y_im = (x_re * h_im + x_im * h_re).astype(BF16)
        conv = dot(b, jnp.concatenate([y_re, y_im], axis=0))
        z = (gate[:, at] * conv).astype(BF16)
        summed[:, to] = z
        if done is not None:
            done(j, to)
        result = dot(lower[...], z)
        last = result[BLOCK - 1 :] * jnp.exp(decay[:, at] * (1.0 - BLOCK))
        for k in range(SUB // 128):
            row = at.start // 128 + k
            state[row : row + 1, :] = last[:, k * 128 : (k + 1) * 128]


def weighted(pieces, place, rate, some=slice(None)):
    out = jnp.zeros(rate.shape, F32)
    for k in range(pieces.shape[0]):
        gap = place - 1 - k
        weight = jnp.exp(-rate * jnp.maximum(gap, 0).astype(F32))
        out = out + jnp.where(gap >= 0, weight * pieces[k, some].astype(F32), 0.0)
    return out


def near_body(place, pieces, rate, inside, copied):
    size, r = pieces.shape[0], rate[...]
    inside[...] = weighted(pieces, place[0], r)
    group = weighted(pieces, jnp.int32(size), r).astype(BF16)
    for k in range(copied.shape[0]):
        copied[k] = group


def early_body(
    summed_far,
    lower,
    outer_far,
    decay,
    scale,
    weights,
    stats,
    sent_far,
    summed,
    long_outer,
    sent,
    *sems,
):
    share = summed.shape[1]
    summed_in = fetches(summed_far, summed, sems[0], 0, PIECE)
    outer_in = fetches(outer_far, long_outer, sems[1], 0, PIECE)
    leaving = []

    def send(low, width):
        at = pl.ds(low, width)
        copy = pltpu.make_async_copy(
            sent.at[:, at], sent_far.at[:, at], sems[2].at[len(leaving)]
        )
        copy.start()
        leaving.append(copy)

    left = stats[...]
    for k in range(3):
        term = left.astype(BF16)
        left = left - term.astype(F32)
        low = 2 * share + k * BLOCK
        sent[:, low : low + BLOCK] = term
    send(2 * share, 3 * BLOCK)
    time = times(PIECE)
    for k, at in enumerate(pieces_of(share, PIECE)):
        d = decay[:, at]
        factor = jnp.exp(-d * time) * scale[:, at]
        summed_in[k].wait()
        base = dot(lower[...], summed[:, at])
        outer_in[k].wait()
        outer = long_outer[:, at].astype(F32) * factor
        value = (outer * base).astype(BF16)
        slope = (outer * jnp.exp(-d)).astype(BF16)
        for j, to in enumerate(pieces_of(PIECE, HEAD_DIM)):
            head = at.start // HEAD_DIM + j
            both = dot(weights[head], jnp.concatenate([value[:, to], slope[:, to]], axis=1))
            low = head * HEAD_DIM
            high = share + low
            sent[:, low : low + HEAD_DIM] = both[:, :HEAD_DIM].astype(BF16)
            sent[:, high : high + HEAD_DIM] = both[:, HEAD_DIM:].astype(BF16)
        send(k * PIECE, PIECE)
        send(share + k * PIECE, PIECE)
    for copy in leaving:
        copy.wait()


def fetch_body(summed_far, outer_far, summed, outer, *sems):
    copies = fetches(summed_far, summed, sems[0], EARLY, PIECE)
    copies += fetches(outer_far, outer, sems[1], EARLY, PIECE)
    for copy in copies:
        copy.wait()


def finish(start, near_size, place, others, inside, rate, lower, decay, scale, mixed, read):
    near, far = place[0], place[1]
    r = rate[...]
    carry = inside[...] + jnp.exp(-r * near.astype(F32)) * weighted(others, far, r * near_size)
    time = times(PIECE)
    for k, to in enumerate(pieces_of(mixed.shape[1], PIECE)):
        at = slice(start + to.start, start + to.stop)
        d = decay[:, at]
        heads = range(at.start // HEAD_DIM, at.stop // HEAD_DIM)
        entering = jnp.concatenate([carry[j : j + 1] for j in heads], axis=1) * jnp.exp(-d)
        factor = jnp.exp(-d * time) * scale[:, at]
        summed, outer = read(k, to)
        base = dot(lower[...], summed) + entering
        mixed[:, to] = (outer.astype(F32) * factor * base).astype(BF16)
    return carry


def finish_first(
    near_size, place, others, inside, rate, summed_far, lower, outer_far, decay, scale, mixed, *rest
):
    summed, outer, summed_sems, outer_sems = rest
    summed_in = fetches(summed_far, summed, summed_sems, 0, PIECE)
    outer_in = fetches(outer_far, outer, outer_sems, 0, PIECE)

    def read(k, to):
        summed_in[k].wait()
        outer_in[k].wait()
        return summed[:, to], outer[:, to]

    finish(0, near_size, place, others, inside, rate, lower, decay, scale, mixed, read)


def partial_attention(start, weights, mixed, ahead):
    for j, to in enumerate(pieces_of(mixed.shape[1], HEAD_DIM)):
        head = start // HEAD_DIM + j
        ahead[:BLOCK, to] = dot(weights[head], mixed[:, to]).astype(BF16)


def finish_middle(
    near_size,
    place,
    others,
    inside,
    rate,
    summed,
    lower,
    outer,
    decay,
    scale,
    weights,
    mixed,
    ahead,
):
    carry = finish(
        EARLY,
        near_size,
        place,
        others,
        inside,
        rate,
        lower,
        decay,
        scale,
        mixed,
        lambda k, to: (summed[:, to], outer[:, to]),
    )
    partial_attention(EARLY, weights, mixed, ahead)
    row = lax.broadcasted_iota(jnp.int32, (16, HEAD_DIM), 0)
    for j, to in enumerate(pieces_of(ahead.shape[1], HEAD_DIM)):
        kept = jnp.zeros((16, HEAD_DIM), F32)
        if to.start < EARLY:
            left = carry[j : j + 1]
            for k in range(3):
                term = left.astype(BF16).astype(F32)
                left = left - term
                kept = jnp.where(row == k, term, kept)
        ahead[BLOCK:, to] = kept.astype(BF16)


def finish_last(
    near_size,
    place,
    others,
    inside,
    rate,
    summed,
    lower,
    outer_far,
    decay,
    scale,
    weights,
    mixed,
    ahead,
    outer,
    sems,
):
    outer_in = fetches(outer_far, outer, sems, MIDDLE, PIECE)

    def read(k, to):
        outer_in[k].wait()
        return summed[:, to], outer[:, to]

    finish(MIDDLE, near_size, place, others, inside, rate, lower, decay, scale, mixed, read)
    partial_attention(MIDDLE, weights, mixed, ahead)


def store_body(first, middle, last, whole, sems):
    leaving, start = [], 0
    for k, block in enumerate((first, middle, last)):
        share = block.shape[1]
        leaving.append(pltpu.make_async_copy(block, whole.at[:, pl.ds(start, share)], sems.at[k]))
        leaving[-1].start()
        start += share
    for copy in leaving:
        copy.wait()


def score(query, key):
    return lax.dot_general(
        query, key, (((1,), (1,)), ((), ())), preferred_element_type=F32
    ) * HEAD_DIM ** (-0.5)


def soft(scores):
    top = jnp.max(scores, axis=1, keepdims=True)
    e = jnp.exp(scores - top)
    return e, top, jnp.sum(e, axis=1, keepdims=True)


def fetches(source, target, sems, first, width):
    copies = []
    for k in range(target.shape[1] // width):
        to = pl.ds(k * width, width)
        at = pl.ds(first + k * width, width)
        copies.append(pltpu.make_async_copy(source.at[:, at], target.at[:, to], sems.at[k]))
    for copy in copies:
        copy.start()
    return copies


def own_body(
    query_far, key_far, weights_far, stats, query, key, weights, query_sems, key_sems, sems
):
    leaving = []
    width = 2 * PIECE
    arriving = [
        pair
        for pair in zip(
            fetches(query_far, query, query_sems, 0, width),
            fetches(key_far, key, key_sems, 0, width),
        )
    ]
    row = lax.broadcasted_iota(jnp.int32, (BLOCK, BLOCK), 0)
    lane = lax.broadcasted_iota(jnp.int32, (BLOCK, BLOCK), 1)
    tops = jnp.zeros((BLOCK, BLOCK), F32)
    sizes = jnp.zeros((BLOCK, BLOCK), F32)
    for j in range(weights.shape[0]):
        at = slice(j * HEAD_DIM, (j + 1) * HEAD_DIM)
        if at.start % width == 0:
            for copy in arriving[at.start // width]:
                copy.wait()
        e, top, size = soft(jnp.where(lane <= row, score(query[:, at], key[:, at]), -1e30))
        weights[j] = e.astype(BF16)
        if (j + 1) % GROUP == 0:
            at = pl.ds(j + 1 - GROUP, GROUP)
            copy = pltpu.make_async_copy(weights.at[at], weights_far.at[at], sems.at[j // GROUP])
            copy.start()
            leaving.append(copy)
        tops = jnp.where(lane == j, top, tops)
        sizes = jnp.where(lane == j + BLOCK // 2, size, sizes)
    stats[...] = jnp.where(lane < BLOCK // 2, tops, sizes)
    for copy in leaving:
        copy.wait()


def ahead_body(query, key_far, weights, stats, key, sems):
    width = 2 * PIECE
    arriving = fetches(key_far, key, sems, 0, width)
    lane = lax.broadcasted_iota(jnp.int32, (BLOCK, BLOCK), 1)
    tops = jnp.zeros((BLOCK, BLOCK), F32)
    sizes = jnp.zeros((BLOCK, BLOCK), F32)
    for j in range(weights.shape[0]):
        at = slice(j * HEAD_DIM, (j + 1) * HEAD_DIM)
        if at.start % width == 0:
            arriving[at.start // width].wait()
        e, top, size = soft(score(query[:, at], key[:, at]))
        weights[j] = (e * (1.0 / size)).astype(BF16)
        tops = jnp.where(lane == j, top, tops)
        sizes = jnp.where(lane == j + BLOCK // 2, size, sizes)
    stats[...] = jnp.where(lane < BLOCK // 2, tops, sizes)


def here_body(
    weights_far, first, middle, last, stats_here, early, base, slope, share, weights, sems
):
    arriving = []
    for k in range(weights.shape[0] // GROUP):
        at = pl.ds(k * GROUP, GROUP)
        arriving.append(pltpu.make_async_copy(weights_far.at[at], weights.at[at], sems.at[k]))
        arriving[-1].start()
    top, size = stats_here[...], pltpu.roll(stats_here[...], BLOCK // 2, 1)
    terms = early[:, 2 * EARLY :].astype(F32)
    stats_before = (terms[:, :BLOCK] + terms[:, BLOCK : 2 * BLOCK]) + terms[:, 2 * BLOCK :]
    size_b = pltpu.roll(stats_before, BLOCK // 2, 1)
    top_b = jnp.where(size_b > 0.0, stats_before, -1e30)
    highest = jnp.maximum(top, top_b)
    scale = jnp.exp(top - highest)
    scale_b = size_b * jnp.exp(top_b - highest)
    whole = 1.0 / (size * scale + scale_b)
    own, other = scale * whole, scale_b * whole
    share[...] = other
    start = 0
    for block in (first, middle, last):
        for to in pieces_of(block.shape[1], HEAD_DIM):
            at = slice(start + to.start, start + to.stop)
            j = at.start // HEAD_DIM
            if j % GROUP == 0:
                arriving[j // GROUP].wait()
            part = dot(weights[j], block[:, to]) * own[:, j : j + 1]
            if start == 0:
                column = other[:, j : j + 1]
                part = part + column * early[:, to].astype(F32)
                up = slice(EARLY + to.start, EARLY + to.stop)
                slope[:, to] = column * early[:, up].astype(F32)
            base[:, at] = part
        start += block.shape[1]


def join_first(base, slope, share, before, attended, out, sems):
    leaving = []
    for k, at in enumerate(pieces_of(MIDDLE, PIECE)):
        for j in range(at.start // HEAD_DIM, at.stop // HEAD_DIM):
            to = slice(j * HEAD_DIM, (j + 1) * HEAD_DIM)
            if to.start < EARLY:
                terms = before[BLOCK:, to].astype(F32)
                more = slope[:, to] * ((terms[:1] + terms[1:2]) + terms[2:3])
            else:
                of = slice(to.start - EARLY, to.stop - EARLY)
                more = share[:, j : j + 1] * before[:BLOCK, of].astype(F32)
            out[:, to] = (base[:, to] + more).astype(BF16)
        at = pl.ds(at.start, PIECE)
        leaving.append(pltpu.make_async_copy(out.at[:, at], attended.at[:, at], sems.at[k]))
        leaving[-1].start()
    for copy in leaving:
        copy.wait()


def join_last(base, share, last, whole, attended, out, sems):
    leaving = []
    for k, to in enumerate(pieces_of(last.shape[1], PIECE)):
        for j in range(to.start // HEAD_DIM, to.stop // HEAD_DIM):
            of = slice(j * HEAD_DIM, (j + 1) * HEAD_DIM)
            at = slice(MIDDLE + of.start, MIDDLE + of.stop)
            head = MIDDLE // HEAD_DIM + j
            value = base[:, at] + share[:, head : head + 1] * last[:, of].astype(F32)
            out[:, of] = value.astype(BF16)
        copy = pltpu.make_async_copy(
            out.at[:, pl.ds(to.start, PIECE)],
            attended.at[:, pl.ds(MIDDLE + to.start, PIECE)],
            sems.at[k],
        )
        copy.start()
        leaving.append(copy)
    for copy in leaving:
        copy.wait()


def on_device(
    stream,
    norm_gain,
    short_outer,
    short_inner,
    short_filter,
    long_outer,
    long_inner,
    long_decay,
    query_heads,
    key_heads,
):
    rows, width = stream.shape
    heads, lanes = width // HEAD_DIM, width // 128
    decay = long_decay[None]
    scale = jnp.sqrt(-jnp.expm1(-2.0 * decay))
    rate = long_decay.reshape(lanes, 128) * rows
    near, far = lax.axis_index(NEAR), lax.axis_index(FAR)
    near_size, far_size = lax.axis_size(NEAR), lax.axis_size(FAR)
    forward, back = jnp.asarray(FORWARD), jnp.asarray(BACK)
    lower = jnp.asarray(np.tril(np.ones((rows, rows), np.float32)), BF16)
    square = ((rows, rows), F32)
    wide, wide_float = ((rows, width), BF16), ((rows, width), F32)

    row_sems = pltpu.SemaphoreType.DMA((rows // ROWS,))
    squares, stream = call(
        squares_body, [((1, rows), F32), wide], [row_sems], operands=1, outside=(0,)
    )(in_hbm(stream))
    beside = swapped(squares)
    v, *sent = call(
        gate_body,
        [wide] + [((rows, share), BF16) for share in TAIL],
        [
            pltpu.VMEM((rows, width), BF16),
            pltpu.VMEM((1, width), F32),
            row_sems,
            pltpu.SemaphoreType.DMA,
        ],
        operands=3,
        outside=(1, 2),
    )(stream, in_hbm(short_inner), in_hbm(norm_gain[None]))
    total, sent[0] = label(squares, beside, sent[0])
    v_before = []
    for part in range(len(TAIL)):
        v_before.append(shifted(sent[part], SEQ, 1))
    queries, total = lax.optimization_barrier((query_heads, total))
    query_next = shifted(queries, SEQ, -1)
    spectrum, gate = call(
        tables_body, [((2 * rows, width), F32), wide_float], operands=5
    )(forward, short_filter, long_inner, short_outer, decay)
    weights_here, stats_here = call(
        own_body,
        [((heads, rows, rows), BF16), square],
        [pltpu.VMEM((rows, width), BF16)] * 2
        + [pltpu.VMEM((heads, rows, rows), BF16)]
        + [pltpu.SemaphoreType.DMA((width // PIECE // 2,))] * 2
        + [pltpu.SemaphoreType.DMA((heads // GROUP,))],
        operands=2,
        outside=(0, 1),
        kept=(0,),
    )(in_hbm(query_heads), in_hbm(key_heads))
    v_before[0], stats_here = lax.optimization_barrier((v_before[0], stats_here))
    summed, state, matrix = call(
        conv_first,
        [((rows, TAIL[0]), BF16), ((TAIL[0] // 128, 128), F32), ((2 * rows, 2 * rows), BF16)],
        [pltpu.VMEM((rows, TAIL[0]), BF16), pltpu.SemaphoreType.DMA((TAIL[0] // SUB,))],
        operands=9,
        kept=(0,),
    )(v_before[0], v, total, forward, back, lower, spectrum, gate, decay)
    summed_last, state = call(
        functools.partial(conv_last, TAIL[0]),
        [((rows, TAIL[1]), BF16), ((near_size, lanes, 128), BF16)],
        [pltpu.VMEM((lanes, 128), F32)],
        operands=9,
    )(v_before[1], v, matrix, back, lower, spectrum, gate, decay, state)
    pieces = lax.all_to_all(state, NEAR, 0, 0, tiled=True)
    weights_next, stats_next = call(
        ahead_body,
        [((heads, rows, rows), BF16), square],
        [pltpu.VMEM((rows, width), BF16), pltpu.SemaphoreType.DMA((width // PIECE // 2,))],
        operands=2,
        outside=(1,),
    )(query_next, in_hbm(key_heads))
    pieces, stats_next = lax.optimization_barrier((pieces, stats_next))
    inside, group = call(
        near_body, [((lanes, 128), F32), ((far_size, lanes, 128), BF16)], scalars=1, operands=2
    )(near[None], pieces, rate)
    others = lax.all_to_all(group, FAR, 0, 0, tiled=True)

    def fetching(share):
        space = [pltpu.VMEM((rows, share), BF16)] * 2
        return space + [pltpu.SemaphoreType.DMA((share // PIECE,))] * 2

    share = MIDDLE - EARLY
    middle_wide, last_wide = ((rows, share), BF16), ((rows, width - MIDDLE), BF16)
    summed, inside = lax.optimization_barrier((summed, inside))
    summed, outer = in_hbm(summed), in_hbm(long_outer)
    (early,) = call(
        early_body,
        [((rows, 2 * EARLY + 3 * rows), BF16)],
        fetching(EARLY)[:2]
        + [pltpu.VMEM((rows, 2 * EARLY + 3 * rows), BF16)]
        + fetching(EARLY)[2:]
        + [pltpu.SemaphoreType.DMA((1 + 2 * EARLY // PIECE,))],
        operands=7,
        outside=(0, 2),
        kept=(0,),
    )(summed, lower, outer, decay, scale, weights_next, stats_next)
    early = shifted(early, SEQ, 1)
    summed_middle, outer_middle = call(
        fetch_body,
        [middle_wide, middle_wide],
        [pltpu.SemaphoreType.DMA((share // PIECE,))] * 2,
        operands=2,
        outside=(0, 1),
    )(summed, outer)
    others, summed_middle = lax.optimization_barrier((others, summed_middle))
    place, steps = jnp.stack([near, far]), float(near_size)
    middle, ready = call(
        functools.partial(finish_middle, steps),
        [middle_wide, ((rows + 16, share), BF16)],
        scalars=1,
        operands=9,
    )(
        place, others, inside, rate, summed_middle, lower, outer_middle, decay, scale, weights_next
    )
    arrived = shifted(ready, SEQ, 1)
    last, ready = call(
        functools.partial(finish_last, steps),
        [last_wide, last_wide],
        [
            pltpu.VMEM((rows, width - MIDDLE), BF16),
            pltpu.SemaphoreType.DMA(((width - MIDDLE) // PIECE,)),
        ],
        scalars=1,
        operands=9,
        outside=(6,),
    )(place, others, inside, rate, summed_last, lower, outer, decay, scale, weights_next)
    arrived_last = shifted(ready, SEQ, 1)
    others, last = lax.optimization_barrier((others, last))
    (first,) = call(
        functools.partial(finish_first, steps),
        [((rows, EARLY), BF16)],
        fetching(EARLY),
        scalars=1,
        operands=8,
        outside=(4, 6),
    )(place, others, inside, rate, summed, lower, outer, decay, scale)
    (values,) = call(
        store_body, [wide], [pltpu.SemaphoreType.DMA((3,))], operands=3, kept=(0,)
    )(first, middle, last)
    base, slope, share = call(
        here_body,
        [wide_float, ((rows, EARLY), F32), square],
        [pltpu.VMEM((heads, rows, rows), BF16), pltpu.SemaphoreType.DMA((heads // GROUP,))],
        operands=6,
        outside=(0,),
    )(in_hbm(weights_here), first, middle, last, stats_here, early)
    (attended,) = call(
        join_first,
        [wide],
        [pltpu.VMEM((rows, MIDDLE), BF16), pltpu.SemaphoreType.DMA((MIDDLE // PIECE,))],
        operands=4,
        kept=(0,),
    )(base, slope, share, arrived)
    (attended,) = call(
        join_last,
        [wide],
        [
            pltpu.VMEM((rows, width - MIDDLE), BF16),
            pltpu.SemaphoreType.DMA(((width - MIDDLE) // PIECE,)),
        ],
        operands=4,
        outside=(3,),
        kept=(0,),
        aliases={3: 0},
    )(base, share, arrived_last, attended)
    return (values, attended)


def solution(mesh):
    finer = Mesh(
        mesh.devices.reshape(8, 2, 4, 2, mesh.shape["mp"]),
        ("seq_0", "seq_1", "seq_2", "seq_3", "mp"),
    )
    placed = (
        P(SEQ, "mp"),
        P("mp"),
        P(SEQ, "mp"),
        P(SEQ, "mp"),
        P(None, "mp"),
        P(SEQ, "mp"),
        P(SEQ, "mp"),
        P("mp"),
        P(SEQ, "mp"),
        P(SEQ, "mp"),
    )
    return jax.shard_map(
        on_device,
        mesh=finer,
        in_specs=placed,
        out_specs=(P(SEQ, "mp"), P(SEQ, "mp")),
        check_vma=False,
    )
```
